32 devices in a mesh: rows: 4 (over y, x), batch: 8 (over z, core).
Axes of the slice: x: 2, y: 2, z: 4, core: 2. Of those that a mesh axis runs over, the one named last changes fastest.
Arguments:
- control: bfloat16 [8, 24, 96, 320], P('batch', 'rows'), may hold values from -60 to 60, as said below
- unet_skips: bfloat16 [2, 8, 24, 96, 320], P(None, 'batch', 'rows'), may hold values from -6 to 6
- norm_gains: float32 [2, 2, 320], replicated, may hold values from 0.25 to 1.75
- norm_shifts: float32 [2, 2, 320], replicated, may hold values from -3 to 3
- conv_weights: bfloat16 [2, 2, 3, 960, 320], P(None, None, None, None, 'batch'), may hold values from -0.109375 to 0.109375
- zero_weights: bfloat16 [2, 1, 320, 320], P(None, None, None, 'batch'), may hold values from -0.3125 to 0.3125
Outputs:
- controls: bfloat16 [2, 8, 24, 96, 320], P(None, 'batch', 'rows')
The draws below stay inside these ranges and needn't reach their ends.
Inputs may be any that keep to these rules, and one draw needn't show every extreme that they name: `control`: Real-valued latent features.
All inputs are finite; a program needn't handle non-finite values.
Results may differ from the reference program's by a relative error of at most 0.01.
Values may be sent and summed in bfloat16 or wider, within the bound.
A program may use at most 64 MiB of HBM per device.

```python
import math
import jax
import jax.numpy as jnp
from jax import lax

C = 320
GROUPS = 32
W = 96
BLOCKS = 2
H = 24
BATCH = 8


def draw_control(key, part):
    first_key = jax.random.fold_in(jax.random.fold_in(key, 17), 0)
    second_key = jax.random.fold_in(jax.random.fold_in(key, 17), 1)
    fourth_key = jax.random.fold_in(jax.random.fold_in(key, 17), 3)
    row_pos = jnp.arange(H, dtype=jnp.float32) / max(H - 1, 1)
    channel_scale = jnp.exp(jax.random.uniform(second_key, (C,), jnp.float32, math.log(0.3), math.log(3.0)))
    channel_offset = jax.random.uniform(fourth_key, (C,), jnp.float32, 0.5, 1.5)
    base = jax.random.truncated_normal(first_key, -6.0, 6.0, (BATCH, H, W, C), jnp.float32)
    row_scale = 1.0 + 2.0 * row_pos
    ramp = 0.5 + 2.5 * row_pos
    values = base * row_scale[None, :, None, None] * channel_scale + ramp[None, :, None, None] * channel_offset
    return values.astype(jnp.bfloat16)


def steps_of(key, dims, cuts, low, largest):
    level = 1.0
    for position, blocks in cuts:
        draws = jax.random.uniform(jax.random.fold_in(jax.random.fold_in(key, 6), position), (blocks,), jnp.float32, low / len(cuts), largest / len(cuts))
        level = level * jnp.repeat(jnp.exp(draws), dims[position] // blocks).reshape((-1,) + (1,) * (len(dims) - 1 - position))
    return level


def gaussian(stream_key, dims, width, reach, cuts=(), kind=jnp.bfloat16):
    result = width * jax.random.normal(stream_key, dims, jnp.float32)
    if cuts:
        result = result * steps_of(stream_key, dims, cuts, -0.22, 0.18)
    return jnp.clip(result, -reach, reach).astype(kind)


def setup_inputs(seed: int = 0) -> dict:
    splits = jax.random.split(jax.random.key(seed), 7)
    return {
        "control": draw_control(jax.random.fold_in(splits[6], 71), 0),
        "unet_skips": gaussian(splits[1], (BLOCKS, BATCH, H, W, C), 1.0, 6.0, ((1, 8), (2, 4))),
        "norm_gains": jnp.clip(1.0 + 0.15 * jax.random.normal(splits[2], (BLOCKS, 2, C), jnp.float32), 0.25, 1.75),
        "norm_shifts": gaussian(splits[3], (BLOCKS, 2, C), 0.5, 3.0, (), jnp.float32),
        "conv_weights": gaussian(splits[4], (BLOCKS, 2, 3, 3 * C, C), (9 * C) ** -0.5, 0.109375, ((4, 8),)),
        "zero_weights": gaussian(splits[5], (BLOCKS, 1, C, C), C ** -0.5, 0.3125, ((3, 8),)),
    }


epsilon = 1e-05

def normalize(values, gain_row, shift_row):
    height, across, channels = values.shape
    grouped = values.astype(jnp.float32).reshape(height, across, GROUPS, channels // GROUPS)
    average = lax.optimization_barrier(jnp.mean(grouped, axis=(0, 1, 3), keepdims=True))
    centered = grouped - average
    spread = lax.optimization_barrier(jnp.mean(centered * centered, axis=(0, 1, 3), keepdims=True))
    scaled = (centered * lax.rsqrt(spread + epsilon)).reshape(height, across, channels) * gain_row + shift_row
    return jax.nn.silu(scaled).astype(jnp.bfloat16)

def convolve(values, weight):
    tap_rows = weight.shape[0]
    tap_cols = weight.shape[1] // values.shape[2]
    margin = tap_rows // 2
    height, across = (values.shape[0], values.shape[1])
    padded = jnp.pad(values, ((margin, margin), (margin, margin), (0, 0)))
    summed = jnp.zeros((height, across, weight.shape[2]), jnp.float32)
    for row_tap in range(tap_rows):
        row_band = padded[row_tap:row_tap + height]
        stacked = jnp.concatenate([row_band[:, col_tap:col_tap + across] for col_tap in range(tap_cols)], axis=2)
        summed = summed + jnp.einsum('hwk,kc->hwc', stacked.astype(jnp.float32), weight[row_tap].astype(jnp.float32))
    return summed

def reference(control, unet_skips, norm_gains, norm_shifts, conv_weights, zero_weights):

    def one_sample(inputs):
        hidden, skip_feats = inputs
        results = []
        for layer_index in range(conv_weights.shape[0]):
            normed = normalize(hidden, norm_gains[layer_index, 0], norm_shifts[layer_index, 0])
            first = convolve(normed, conv_weights[layer_index, 0]).astype(jnp.bfloat16)
            normed_two = normalize(first, norm_gains[layer_index, 1], norm_shifts[layer_index, 1])
            second = convolve(normed_two, conv_weights[layer_index, 1])
            hidden = (hidden.astype(jnp.float32) + second).astype(jnp.bfloat16)
            zeroed = convolve(hidden, zero_weights[layer_index])
            results.append((zeroed + skip_feats[layer_index].astype(jnp.float32)).astype(jnp.bfloat16))
        return jnp.stack(results)
    stacked_out = lax.map(one_sample, (control, jnp.moveaxis(unet_skips, 0, 1)))
    return jnp.moveaxis(stacked_out, 0, 1)
```

```python
import functools

import jax
import jax.numpy as jnp
from jax import lax
from jax.experimental import pallas as pl
from jax.experimental.pallas import tpu as pltpu
from jax.sharding import PartitionSpec as P

GROUPS = 32
EPSILON = 1e-05
MESH = pl.DeviceIdType.MESH
LOOKAHEAD = 3
TO_B, TO_D = 2, 4


def transposed(conv_weights, zero_weights):
    blocks, convs, taps, depth, outs = conv_weights.shape
    conv = jnp.transpose(conv_weights, (0, 1, 2, 4, 3)).reshape(blocks * convs * taps, outs, depth)
    return conv, jnp.transpose(zero_weights[:, 0], (0, 2, 1))


def kernel(dims, x_hbm, skip_hbm, gain_hbm, shift_hbm, w_hbm, zw_hbm, out_ref,
           xv, skipv, gainv, shiftv, wv, zwv, group, slabs, wfull, zfull, stk, acc, halo, fields,
           stat_out, stat_in, load,
           z_send, z_recv, a_send, a_recv, b_send, b_recv, d_send, d_recv,
           h_send, h_recv, t_send, t_recv):
    rows_n, batch_n, height, across, channels, outs, taps, members = dims
    units, _, depth = w_hbm.shape
    blocks = zw_hbm.shape[0]
    convs = units // taps
    per_block = convs // blocks
    lanes = slabs.shape[3]
    piece = lanes - depth
    pieces = -(-channels // piece)
    cells = height * across
    zn = batch_n // 2
    r = lax.axis_index("rows")
    b = lax.axis_index("batch")
    z, c = b // 2, b % 2
    bit0, bit1 = r % 2, (r // 2) % 2
    px, py = r + 1 - 2 * bit0, r + 2 - 4 * bit1
    mate = b + 1 - 2 * c
    quarter, eighth = lanes // 4, lanes // 8
    g = bit0 * (1 + bit1) + (1 - bit0) * 3 * bit1
    gx = g + 1 - 2 * (g % 2)
    gy = 3 - g
    even = (g + g % 2) % 4
    odd = g + 1 - g % 2

    def part(index):
        return pl.ds(pl.multiple_of(index * quarter, quarter), quarter)

    def first(index):
        return pl.ds(pl.multiple_of(index * quarter, eighth), eighth)

    def second(index):
        return pl.ds(pl.multiple_of(index * quarter + eighth, eighth), eighth)

    def plane(m):
        other, weight = 0, 1
        while weight < zn:
            other = other + ((z // weight + m // weight) % 2) * weight
            weight *= 2
        return other

    def slab(m):
        return plane(m) * 2 + c

    far = list(range(zn - 1, 1, -1))

    def remote(src, dst, send, recv, row, batch):
        return pltpu.make_async_remote_copy(
            src_ref=src, dst_ref=dst, send_sem=send, recv_sem=recv,
            device_id={"rows": row, "batch": batch}, device_id_type=MESH)

    barrier = pltpu.get_barrier_semaphore()
    for j in range(1, zn):
        pl.semaphore_signal(barrier, inc=1, device_id_type=MESH,
                            device_id={"rows": r, "batch": ((z + j) % zn) * 2 + c})
    for j in range(1, rows_n):
        pl.semaphore_signal(barrier, inc=1, device_id_type=MESH,
                            device_id={"rows": (r + j) % rows_n, "batch": b})
    pl.semaphore_signal(barrier, inc=1, device_id_type=MESH, device_id={"rows": r, "batch": mate})

    loads = [
        pltpu.make_async_copy(w_hbm.at[pl.ds(0, taps)], wv.at[pl.ds(0, taps)], load.at[0]),
        pltpu.make_async_copy(zw_hbm, zwv, load.at[1]),
        pltpu.make_async_copy(x_hbm, xv, load.at[2]),
        pltpu.make_async_copy(w_hbm.at[pl.ds(taps, units - taps)], wv.at[pl.ds(taps, units - taps)],
                              load.at[3]),
        pltpu.make_async_copy(gain_hbm, gainv, load.at[4]),
        pltpu.make_async_copy(shift_hbm, shiftv, load.at[5]),
        pltpu.make_async_copy(skip_hbm, skipv, load.at[6]),
    ]
    for copy in loads:
        copy.start()

    def pack(u):
        block, p = u // (per_block * taps), u % (per_block * taps)
        slabs[u, b, :, :depth] = wv[u]
        if p < pieces:
            wide = min(piece, channels - p * piece)
            slabs[u, b, :, depth:depth + wide] = zwv[block, :, p * piece:p * piece + wide]

    def z_step(u):
        for m in far:
            here = slabs.at[u, b, :, part(g)]
            remote(here, here, z_send.at[u], z_recv.at[u], r, slab(m)).start()
        for index in (even, odd):
            here = slabs.at[u, b, :, part(index)]
            remote(here, here, z_send.at[u], z_recv.at[u], r, slab(1)).start()

    def own_step(u):
        here = slabs.at[u, b]
        remote(here, here, d_send.at[u], d_recv.at[u], r, mate).start()

    def totals(u):
        return (
            (slabs.at[u, pl.ds(0, zn), :, pl.ds(0, quarter)], z_send, z_recv),
            (slabs.at[u, pl.ds(0, zn - 1), :, pl.ds(0, 2 * quarter)], a_send, a_recv),
            (slabs.at[u, pl.ds(0, zn - 2), :, pl.ds(0, quarter)], b_send, b_recv),
            (slabs.at[u, pl.ds(0, zn)], d_send, d_recv),
        )

    def arrived(u, stage):
        ref, send, recv = totals(u)[stage]
        remote(ref, ref, send.at[u], recv.at[u], r, mate).wait_recv()

    def a_step(u):
        arrived(u, 0)
        for m in far:
            here = slabs.at[u, slab(m), :, part(g)]
            remote(here, here, a_send.at[u], a_recv.at[u], px, b).start()
            remote(here, here, a_send.at[u], a_recv.at[u], py, b).start()
        here = slabs.at[u, slab(1), :, part(even)]
        remote(here, here, a_send.at[u], a_recv.at[u], px, b).start()
        here = slabs.at[u, slab(1), :, part(odd)]
        remote(here, here, a_send.at[u], a_recv.at[u], py, b).start()

    def b_step(u):
        arrived(u, 1)
        for m in far:
            here = slabs.at[u, slab(m), :, first(gy)]
            remote(here, here, b_send.at[u], b_recv.at[u], px, b).start()
            here = slabs.at[u, slab(m), :, second(gx)]
            remote(here, here, b_send.at[u], b_recv.at[u], py, b).start()
        here = slabs.at[u, slab(1)]
        remote(here, here, d_send.at[u], d_recv.at[u], r, mate).start()

    def d_step(u):
        if far:
            arrived(u, 2)
        for m in far:
            here = slabs.at[u, slab(m)]
            remote(here, here, d_send.at[u], d_recv.at[u], r, mate).start()

    done = [0]

    def advance(count=1):
        for _ in range(min(count, units + TO_D - done[0])):
            j = done[0]
            done[0] += 1
            if 0 <= j - TO_D:
                d_step(j - TO_D)
            if 0 <= j - TO_B < units:
                b_step(j - TO_B)
            if j < units:
                a_step(j)
            if j + LOOKAHEAD < units:
                z_step(j + LOOKAHEAD)

    def assemble(u):
        arrived(u, 3)
        for d in range(batch_n):
            wfull[u % taps, d * outs:(d + 1) * outs, :] = slabs[u, d, :, :depth]

    def assemble_zero(block):
        for d in range(batch_n):
            parts = []
            for p in range(pieces):
                wide = min(piece, channels - p * piece)
                parts.append(slabs[block * per_block * taps + p, d, :, depth:depth + wide])
            zfull[d * outs:(d + 1) * outs, :] = jnp.concatenate(parts, axis=1)

    def times(a, w):
        return lax.dot_general(a, w, (((1,), (1,)), ((), ())), preferred_element_type=jnp.float32)

    def halo_copies(s, ref):
        def down():
            return remote(ref.at[pl.ds(cells - across, across)], halo.at[s, 0],
                          h_send.at[s, 0], h_recv.at[s, 0], (r + 1) % rows_n, b)

        def up():
            return remote(ref.at[pl.ds(0, across)], halo.at[s, 1],
                          h_send.at[s, 1], h_recv.at[s, 1], (r + rows_n - 1) % rows_n, b)

        return down, up

    def halo_start(s, ref):
        down, up = halo_copies(s, ref)

        @pl.when(r < rows_n - 1)
        def _():
            down().start()

        @pl.when(r > 0)
        def _():
            up().start()

        return down, up

    sent = []

    def stat_start(s, total, square):
        stat_out[s] = jnp.concatenate([total, square, jnp.zeros((6, channels), jnp.float32)], axis=0)
        for j in range(1, rows_n):
            copy = remote(stat_out.at[s], stat_in.at[s, j], t_send.at[s, j], t_recv.at[s, j],
                          (r + j) % rows_n, b)
            copy.start()
            sent.append(copy)

    col = lax.broadcasted_iota(jnp.int32, (across, channels), 0)

    def normalize(s, ref, ends):
        total = stat_out[s]
        for j in range(1, rows_n):
            here = stat_in.at[s, j]
            remote(here, here, t_send.at[s, j], t_recv.at[s, j], r, mate).wait_recv()
            total = total + stat_in[s, j]
        high = total.astype(jnp.bfloat16).astype(jnp.float32)
        rest = total - high
        middle = rest.astype(jnp.bfloat16).astype(jnp.float32)
        split = jnp.concatenate([high, middle, rest - middle], axis=0).astype(jnp.bfloat16)
        grouped = jnp.dot(split, group[...], preferred_element_type=jnp.float32)
        grouped = (grouped[0:8] + grouped[8:16] + grouped[16:24]) * (1.0 / members)
        mean = grouped[0:1]
        spread = jnp.maximum(grouped[1:2] - mean * mean, 0.0)
        block, half = s // per_block, s % per_block
        scale = lax.rsqrt(spread + EPSILON) * gainv[block, half:half + 1, :]
        bias = shiftv[block, half:half + 1, :] - mean * scale

        def put(at, v, valid):
            y = v.astype(jnp.float32) * scale + bias
            a = y / (1.0 + jnp.exp(-y))
            if valid is not None:
                a = jnp.where(valid, a, 0.0)
            left = jnp.where(col == 0, 0.0, pltpu.roll(a, 1, 0))
            right = jnp.where(col == across - 1, 0.0, pltpu.roll(a, across - 1, 0))
            stk[pl.ds(at, across), :] = jnp.concatenate(
                [left.astype(jnp.bfloat16), a.astype(jnp.bfloat16), right.astype(jnp.bfloat16)], axis=1)

        def body(i, carry):
            at = pl.multiple_of(i * across, across)
            put(pl.multiple_of(at + across, across), ref[pl.ds(at, across), :], None)
            return carry
        lax.fori_loop(0, height, body, 0)

        down, up = ends

        @pl.when(r > 0)
        def _():
            down().wait_recv()

        @pl.when(r < rows_n - 1)
        def _():
            up().wait_recv()

        put(0, halo[s, 0], r > 0)
        put((height + 1) * across, halo[s, 1], r < rows_n - 1)

    def keep(s, source, at, value):
        size = value.shape[0]
        if source is not None:
            value = source[at:at + size, :].astype(jnp.float32) + value
        value = value.astype(jnp.bfloat16)
        fields[s, at:at + size, :] = value
        kept = value.astype(jnp.float32)
        return (jnp.sum(kept, axis=0, keepdims=True),
                jnp.sum(kept * kept, axis=0, keepdims=True))

    def convolve(s, source):
        last = taps - 1
        for t in range(taps):
            advance(s * taps + t + TO_D + 1 - done[0])
            assemble(s * taps + t)
            if t == last:
                break
            value = times(stk[t * across:t * across + cells, :], wfull[t])
            acc[...] = value if t == 0 else acc[...] + value
            if t == 0:
                advance()
        low, high = last * across, (height - 1 + last) * across
        both = jnp.concatenate([stk[low:low + across, :], stk[high:high + across, :]], axis=0)
        border = times(both, wfull[last])
        top = keep(s, source, 0, acc[0:across, :] + border[:across])
        bottom = keep(s, source, cells - across, acc[cells - across:, :] + border[across:])
        if s + 1 < convs:
            ends.append(halo_start(s + 1, fields.at[s]))
        inner = times(stk[low + across:high, :], wfull[last])
        middle = keep(s, source, across, acc[across:cells - across, :] + inner)
        return middle[0] + top[0] + bottom[0], middle[1] + top[1] + bottom[1]

    def zero_conv(s):
        block = s // per_block
        assemble_zero(block)
        zeroed = times(fields[s], zfull[...])
        out_ref[block] = (skipv[block].astype(jnp.float32) + zeroed).astype(jnp.bfloat16)

    per = channels // GROUPS
    same = (lax.broadcasted_iota(jnp.int32, (channels, channels), 0) // per
            == lax.broadcasted_iota(jnp.int32, (channels, channels), 1) // per)
    group[...] = jnp.where(same, 1.0, 0.0).astype(jnp.bfloat16)

    loads[0].wait()
    loads[1].wait()
    for u in range(taps):
        pack(u)
    pl.semaphore_wait(barrier, zn + rows_n - 1)
    for u in range(min(LOOKAHEAD, units)):
        z_step(u)
        own_step(u)
    loads[2].wait()
    ends = [halo_start(0, xv)]
    whole = xv[...].astype(jnp.float32)
    stat_start(0, jnp.sum(whole, axis=0, keepdims=True), jnp.sum(whole * whole, axis=0, keepdims=True))
    loads[3].wait()
    for u in range(taps, units):
        pack(u)
    for u in range(min(LOOKAHEAD, units), units):
        own_step(u)
    for copy in loads[4:]:
        copy.wait()
    advance(1)
    normalize(0, xv, ends[0])
    advance(TO_D)
    source = xv
    for s in range(convs):
        if s > 0:
            advance()
            normalize(s, fields.at[s - 1], ends[s])
            advance()
        last = s % per_block == per_block - 1
        sums = convolve(s, source if last else None)
        if s < convs - 1:
            stat_start(s + 1, *sums)
        if last:
            source = fields.at[s]
            zero_conv(s)
    advance(units)
    for copy in sent:
        copy.wait_send()
    for u in range(units):
        for stage, (ref, send, recv) in enumerate(totals(u)):
            if far or stage != 2:
                remote(ref, ref, send.at[u], recv.at[u], r, mate).wait_send()
    for down, up in ends:
        @pl.when(r < rows_n - 1)
        def _():
            down().wait_send()

        @pl.when(r > 0)
        def _():
            up().wait_send()


def on_device(rows_n, batch_n, control, unet_skips, norm_gains, norm_shifts, conv_weights, zero_weights):
    blocks, convs, taps, depth, outs = conv_weights.shape
    samples, height, across, channels = control.shape
    lanes = (depth // 512 + 1) * 512
    stages = blocks * convs
    units = stages * taps
    cells = height * across
    per = channels // GROUPS
    conv, zero = transposed(conv_weights, zero_weights)
    members = cells * rows_n * per
    dims = (rows_n, batch_n, height, across, channels, outs, taps, members)
    dma = pltpu.SemaphoreType.DMA
    hbm = pl.BlockSpec(memory_space=pltpu.HBM)
    out = pl.pallas_call(
        functools.partial(kernel, dims),
        out_shape=jax.ShapeDtypeStruct((blocks, cells, channels), jnp.bfloat16),
        in_specs=[hbm] * 6,
        out_specs=pl.BlockSpec(memory_space=pltpu.VMEM),
        scratch_shapes=[
            pltpu.VMEM((cells, channels), jnp.bfloat16),
            pltpu.VMEM((blocks, cells, channels), jnp.bfloat16),
            pltpu.VMEM((blocks, convs, channels), jnp.float32),
            pltpu.VMEM((blocks, convs, channels), jnp.float32),
            pltpu.VMEM((units, outs, depth), jnp.bfloat16),
            pltpu.VMEM((blocks, outs, channels), jnp.bfloat16),
            pltpu.VMEM((channels, channels), jnp.bfloat16),
            pltpu.VMEM((units, batch_n, outs, lanes), jnp.bfloat16),
            pltpu.VMEM((taps, channels, depth), jnp.bfloat16),
            pltpu.VMEM((channels, channels), jnp.bfloat16),
            pltpu.VMEM(((height + taps - 1) * across, depth), jnp.bfloat16),
            pltpu.VMEM((cells, channels), jnp.float32),
            pltpu.VMEM((stages, 2, across, channels), jnp.bfloat16),
            pltpu.VMEM((stages, cells, channels), jnp.bfloat16),
            pltpu.VMEM((stages, 8, channels), jnp.float32),
            pltpu.VMEM((stages, rows_n, 8, channels), jnp.float32),
            dma((7,)),
            dma((units,)), dma((units,)),
            dma((units,)), dma((units,)),
            dma((units,)), dma((units,)),
            dma((units,)), dma((units,)),
            dma((stages, 2)), dma((stages, 2)),
            dma((stages, rows_n)), dma((stages, rows_n)),
        ],
        compiler_params=pltpu.CompilerParams(
            collective_id=0, has_side_effects=True, vmem_limit_bytes=50 * 1024 * 1024),
    )(
        control.reshape(cells, channels),
        unet_skips.reshape(blocks, cells, channels),
        norm_gains,
        norm_shifts,
        conv,
        zero,
    )
    return out.reshape(blocks, samples, height, across, channels)


def solution(mesh):
    placed = (
        P("batch", "rows", None, None),
        P(None, "batch", "rows", None, None),
        P(),
        P(),
        P(None, None, None, None, "batch"),
        P(None, None, None, "batch"),
    )
    return jax.shard_map(
        functools.partial(on_device, mesh.shape["rows"], mesh.shape["batch"]),
        mesh=mesh,
        in_specs=placed,
        out_specs=P(None, "batch", "rows", None, None),
        check_vma=False,
    )
```

```python
import functools

import jax
import jax.numpy as jnp
from jax import lax
from jax.experimental import pallas as pl
from jax.experimental.pallas import tpu as pltpu
from jax.sharding import PartitionSpec as P

GROUPS = 32
EPSILON = 1e-05
MESH = pl.DeviceIdType.MESH
LOOKAHEAD = 3
TO_B, TO_D = 2, 4


def transposed(conv_weights, zero_weights):
    blocks, convs, taps, depth, outs = conv_weights.shape
    conv = jnp.transpose(conv_weights, (0, 1, 2, 4, 3)).reshape(blocks * convs * taps, outs, depth)
    return conv, jnp.transpose(zero_weights[:, 0], (0, 2, 1))


def kernel(dims, x_hbm, skip_hbm, gain_hbm, shift_hbm, w_hbm, zw_hbm, out_ref,
           xv, skipv, gainv, shiftv, wv, zwv, group, slabs, wfull, zfull, stk, acc, halo, fields,
           stat_out, stat_in, load,
           z_send, z_recv, a_send, a_recv, b_send, b_recv, d_send, d_recv,
           h_send, h_recv, t_send, t_recv):
    rows_n, batch_n, height, across, channels, outs, taps, members = dims
    units, _, depth = w_hbm.shape
    blocks = zw_hbm.shape[0]
    convs = units // taps
    per_block = convs // blocks
    lanes = slabs.shape[3]
    piece = lanes - depth
    pieces = -(-channels // piece)
    cells = height * across
    zn = batch_n // 2
    r = lax.axis_index("rows")
    b = lax.axis_index("batch")
    z, c = b // 2, b % 2
    bit0, bit1 = r % 2, (r // 2) % 2
    px, py = r + 1 - 2 * bit0, r + 2 - 4 * bit1
    mate = b + 1 - 2 * c
    quarter, eighth = lanes // 4, lanes // 8
    g = bit0 * (1 + bit1) + (1 - bit0) * 3 * bit1
    gx = g + 1 - 2 * (g % 2)
    gy = 3 - g
    even = (g + g % 2) % 4
    odd = g + 1 - g % 2

    def part(index):
        return pl.ds(pl.multiple_of(index * quarter, quarter), quarter)

    def first(index):
        return pl.ds(pl.multiple_of(index * quarter, eighth), eighth)

    def second(index):
        return pl.ds(pl.multiple_of(index * quarter + eighth, eighth), eighth)

    def plane(m):
        other, weight = 0, 1
        while weight < zn:
            other = other + ((z // weight + m // weight) % 2) * weight
            weight *= 2
        return other

    def slab(m):
        return plane(m) * 2 + c

    far = list(range(zn - 1, 1, -1))

    def remote(src, dst, send, recv, row, batch):
        return pltpu.make_async_remote_copy(
            src_ref=src, dst_ref=dst, send_sem=send, recv_sem=recv,
            device_id={"rows": row, "batch": batch}, device_id_type=MESH)

    barrier = pltpu.get_barrier_semaphore()
    for j in range(1, zn):
        pl.semaphore_signal(barrier, inc=1, device_id_type=MESH,
                            device_id={"rows": r, "batch": ((z + j) % zn) * 2 + c})
    for j in range(1, rows_n):
        pl.semaphore_signal(barrier, inc=1, device_id_type=MESH,
                            device_id={"rows": (r + j) % rows_n, "batch": b})
    pl.semaphore_signal(barrier, inc=1, device_id_type=MESH, device_id={"rows": r, "batch": mate})

    loads = [
        pltpu.make_async_copy(w_hbm.at[pl.ds(0, taps)], wv.at[pl.ds(0, taps)], load.at[0]),
        pltpu.make_async_copy(zw_hbm, zwv, load.at[1]),
        pltpu.make_async_copy(x_hbm, xv, load.at[2]),
        pltpu.make_async_copy(w_hbm.at[pl.ds(taps, units - taps)], wv.at[pl.ds(taps, units - taps)],
                              load.at[3]),
        pltpu.make_async_copy(gain_hbm, gainv, load.at[4]),
        pltpu.make_async_copy(shift_hbm, shiftv, load.at[5]),
        pltpu.make_async_copy(skip_hbm, skipv, load.at[6]),
    ]
    for copy in loads:
        copy.start()

    def pack(u):
        block, p = u // (per_block * taps), u % (per_block * taps)
        slabs[u, b, :, :depth] = wv[u]
        if p < pieces:
            wide = min(piece, channels - p * piece)
            slabs[u, b, :, depth:depth + wide] = zwv[block, :, p * piece:p * piece + wide]

    def z_step(u):
        for m in far:
            here = slabs.at[u, b, :, part(g)]
            remote(here, here, z_send.at[u], z_recv.at[u], r, slab(m)).start()
        for index in (even, odd):
            here = slabs.at[u, b, :, part(index)]
            remote(here, here, z_send.at[u], z_recv.at[u], r, slab(1)).start()

    def own_step(u):
        here = slabs.at[u, b]
        remote(here, here, d_send.at[u], d_recv.at[u], r, mate).start()

    def totals(u):
        return (
            (slabs.at[u, pl.ds(0, zn), :, pl.ds(0, quarter)], z_send, z_recv),
            (slabs.at[u, pl.ds(0, zn - 1), :, pl.ds(0, 2 * quarter)], a_send, a_recv),
            (slabs.at[u, pl.ds(0, zn - 2), :, pl.ds(0, quarter)], b_send, b_recv),
            (slabs.at[u, pl.ds(0, zn)], d_send, d_recv),
        )

    def arrived(u, stage):
        ref, send, recv = totals(u)[stage]
        remote(ref, ref, send.at[u], recv.at[u], r, mate).wait_recv()

    def a_step(u):
        arrived(u, 0)
        for m in far:
            here = slabs.at[u, slab(m), :, part(g)]
            remote(here, here, a_send.at[u], a_recv.at[u], px, b).start()
            remote(here, here, a_send.at[u], a_recv.at[u], py, b).start()
        here = slabs.at[u, slab(1), :, part(even)]
        remote(here, here, a_send.at[u], a_recv.at[u], px, b).start()
        here = slabs.at[u, slab(1), :, part(odd)]
        remote(here, here, a_send.at[u], a_recv.at[u], py, b).start()

    def b_step(u):
        arrived(u, 1)
        for m in far:
            here = slabs.at[u, slab(m), :, first(gy)]
            remote(here, here, b_send.at[u], b_recv.at[u], px, b).start()
            here = slabs.at[u, slab(m), :, second(gx)]
            remote(here, here, b_send.at[u], b_recv.at[u], py, b).start()
        here = slabs.at[u, slab(1)]
        remote(here, here, d_send.at[u], d_recv.at[u], r, mate).start()

    def d_step(u):
        if far:
            arrived(u, 2)
        for m in far:
            here = slabs.at[u, slab(m)]
            remote(here, here, d_send.at[u], d_recv.at[u], r, mate).start()

    done = [0]

    def advance(count=1):
        for _ in range(min(count, units + TO_D - done[0])):
            j = done[0]
            done[0] += 1
            if 0 <= j - TO_D:
                d_step(j - TO_D)
            if 0 <= j - TO_B < units:
                b_step(j - TO_B)
            if j < units:
                a_step(j)
            if j + LOOKAHEAD < units:
                z_step(j + LOOKAHEAD)

    def assemble(u):
        arrived(u, 3)
        for d in range(batch_n):
            wfull[u % taps, d * outs:(d + 1) * outs, :] = slabs[u, d, :, :depth]

    def assemble_zero(block):
        for d in range(batch_n):
            parts = []
            for p in range(pieces):
                wide = min(piece, channels - p * piece)
                parts.append(slabs[block * per_block * taps + p, d, :, depth:depth + wide])
            zfull[d * outs:(d + 1) * outs, :] = jnp.concatenate(parts, axis=1)

    def times(a, w):
        return lax.dot_general(a, w, (((1,), (1,)), ((), ())), preferred_element_type=jnp.float32)

    def halo_copies(s, ref):
        def down():
            return remote(ref.at[pl.ds(cells - across, across)], halo.at[s, 0],
                          h_send.at[s, 0], h_recv.at[s, 0], (r + 1) % rows_n, b)

        def up():
            return remote(ref.at[pl.ds(0, across)], halo.at[s, 1],
                          h_send.at[s, 1], h_recv.at[s, 1], (r + rows_n - 1) % rows_n, b)

        return down, up

    def halo_start(s, ref):
        down, up = halo_copies(s, ref)

        @pl.when(r < rows_n - 1)
        def _():
            down().start()

        @pl.when(r > 0)
        def _():
            up().start()

        return down, up

    sent = []

    def stat_start(s, total, square):
        stat_out[s] = jnp.concatenate([total, square, jnp.zeros((6, channels), jnp.float32)], axis=0)
        for j in range(1, rows_n):
            copy = remote(stat_out.at[s], stat_in.at[s, j], t_send.at[s, j], t_recv.at[s, j],
                          (r + j) % rows_n, b)
            copy.start()
            sent.append(copy)

    col = lax.broadcasted_iota(jnp.int32, (across, channels), 0)

    def normalize(s, ref):
        total = stat_out[s]
        for j in range(1, rows_n):
            here = stat_in.at[s, j]
            remote(here, here, t_send.at[s, j], t_recv.at[s, j], r, mate).wait_recv()
            total = total + stat_in[s, j]
        high = total.astype(jnp.bfloat16).astype(jnp.float32)
        rest = total - high
        middle = rest.astype(jnp.bfloat16).astype(jnp.float32)
        split = jnp.concatenate([high, middle, rest - middle], axis=0).astype(jnp.bfloat16)
        grouped = jnp.dot(split, group[...], preferred_element_type=jnp.float32)
        grouped = (grouped[0:8] + grouped[8:16] + grouped[16:24]) * (1.0 / members)
        mean = grouped[0:1]
        spread = jnp.maximum(grouped[1:2] - mean * mean, 0.0)
        block, half = s // per_block, s % per_block
        scale = lax.rsqrt(spread + EPSILON) * gainv[block, half:half + 1, :]
        bias = shiftv[block, half:half + 1, :] - mean * scale

        def put(at, v, valid):
            y = v.astype(jnp.float32) * scale + bias
            a = y / (1.0 + jnp.exp(-y))
            if valid is not None:
                a = jnp.where(valid, a, 0.0)
            left = jnp.where(col == 0, 0.0, pltpu.roll(a, 1, 0))
            right = jnp.where(col == across - 1, 0.0, pltpu.roll(a, across - 1, 0))
            stk[pl.ds(at, across), :] = jnp.concatenate(
                [left.astype(jnp.bfloat16), a.astype(jnp.bfloat16), right.astype(jnp.bfloat16)], axis=1)

        def body(i, carry):
            at = pl.multiple_of(i * across, across)
            put(pl.multiple_of(at + across, across), ref[pl.ds(at, across), :], None)
            return carry
        lax.fori_loop(0, height, body, 0)

        return put

    def edges(s, put):
        down, up = ends[s]

        @pl.when(r > 0)
        def _():
            down().wait_recv()

        @pl.when(r < rows_n - 1)
        def _():
            up().wait_recv()

        put(0, halo[s, 0], r > 0)
        put((height + 1) * across, halo[s, 1], r < rows_n - 1)

    def keep(s, source, at, value):
        size = value.shape[0]
        if source is not None:
            value = source[at:at + size, :].astype(jnp.float32) + value
        value = value.astype(jnp.bfloat16)
        fields[s, at:at + size, :] = value
        kept = value.astype(jnp.float32)
        return (jnp.sum(kept, axis=0, keepdims=True),
                jnp.sum(kept * kept, axis=0, keepdims=True))

    def convolve(s, source, put):
        units_of = range(s * taps, (s + 1) * taps)
        rows = cells - 2 * across
        if s == 0:
            for t, u in enumerate(units_of):
                advance(u + TO_D + 1 - done[0])
                assemble(u)
                value = times(stk[(t + 1) * across:(t + 1) * across + rows, :], wfull[t])
                if t < taps - 1:
                    acc[...] = value if t == 0 else acc[...] + value
            inner = acc[...] + value
        else:
            for u in units_of:
                advance(u + TO_D + 1 - done[0])
                assemble(u)
            inner = None
            for t in range(taps):
                value = times(stk[(t + 1) * across:(t + 1) * across + rows, :], wfull[t])
                inner = value if t == 0 else inner + value
        middle = keep(s, source, across, inner)
        advance()
        edges(s, put)
        border = None
        for t in range(taps):
            low, high = t * across, (height - 1 + t) * across
            both = jnp.concatenate([stk[low:low + across, :], stk[high:high + across, :]], axis=0)
            value = times(both, wfull[t])
            border = value if t == 0 else border + value
        top = keep(s, source, 0, border[:across])
        bottom = keep(s, source, cells - across, border[across:])
        return middle[0] + top[0] + bottom[0], middle[1] + top[1] + bottom[1]

    def zero_conv(s):
        block = s // per_block
        assemble_zero(block)
        zeroed = times(fields[s], zfull[...])
        out_ref[block] = (skipv[block].astype(jnp.float32) + zeroed).astype(jnp.bfloat16)

    per = channels // GROUPS
    same = (lax.broadcasted_iota(jnp.int32, (channels, channels), 0) // per
            == lax.broadcasted_iota(jnp.int32, (channels, channels), 1) // per)
    group[...] = jnp.where(same, 1.0, 0.0).astype(jnp.bfloat16)

    loads[2].wait()
    whole = xv[...].astype(jnp.float32)
    sums = (jnp.sum(whole, axis=0, keepdims=True), jnp.sum(whole * whole, axis=0, keepdims=True))
    loads[0].wait()
    loads[1].wait()
    for u in range(taps):
        pack(u)
    pl.semaphore_wait(barrier, zn + rows_n - 1)
    for u in range(min(LOOKAHEAD, units)):
        z_step(u)
    stat_start(0, *sums)
    ends = [halo_start(0, xv)]
    for u in range(min(LOOKAHEAD, units)):
        own_step(u)
    loads[3].wait()
    for u in range(taps, units):
        pack(u)
    for u in range(min(LOOKAHEAD, units), units):
        own_step(u)
    for copy in loads[4:]:
        copy.wait()
    put = normalize(0, xv)
    advance(TO_D + 1)
    source = xv
    for s in range(convs):
        if s > 0:
            advance(2)
            put = normalize(s, fields.at[s - 1])
        last = s % per_block == per_block - 1
        sums = convolve(s, source if last else None, put)
        if s < convs - 1:
            stat_start(s + 1, *sums)
            ends.append(halo_start(s + 1, fields.at[s]))
        if last:
            source = fields.at[s]
            zero_conv(s)
    advance(units)
    for copy in sent:
        copy.wait_send()
    for u in range(units):
        for stage, (ref, send, recv) in enumerate(totals(u)):
            if far or stage != 2:
                remote(ref, ref, send.at[u], recv.at[u], r, mate).wait_send()
    for down, up in ends:
        @pl.when(r < rows_n - 1)
        def _():
            down().wait_send()

        @pl.when(r > 0)
        def _():
            up().wait_send()


def on_device(rows_n, batch_n, control, unet_skips, norm_gains, norm_shifts, conv_weights, zero_weights):
    blocks, convs, taps, depth, outs = conv_weights.shape
    samples, height, across, channels = control.shape
    lanes = (depth // 512 + 1) * 512
    stages = blocks * convs
    units = stages * taps
    cells = height * across
    per = channels // GROUPS
    conv, zero = transposed(conv_weights, zero_weights)
    members = cells * rows_n * per
    dims = (rows_n, batch_n, height, across, channels, outs, taps, members)
    dma = pltpu.SemaphoreType.DMA
    hbm = pl.BlockSpec(memory_space=pltpu.HBM)
    out = pl.pallas_call(
        functools.partial(kernel, dims),
        out_shape=jax.ShapeDtypeStruct((blocks, cells, channels), jnp.bfloat16),
        in_specs=[hbm] * 6,
        out_specs=pl.BlockSpec(memory_space=pltpu.VMEM),
        scratch_shapes=[
            pltpu.VMEM((cells, channels), jnp.bfloat16),
            pltpu.VMEM((blocks, cells, channels), jnp.bfloat16),
            pltpu.VMEM((blocks, convs, channels), jnp.float32),
            pltpu.VMEM((blocks, convs, channels), jnp.float32),
            pltpu.VMEM((units, outs, depth), jnp.bfloat16),
            pltpu.VMEM((blocks, outs, channels), jnp.bfloat16),
            pltpu.VMEM((channels, channels), jnp.bfloat16),
            pltpu.VMEM((units, batch_n, outs, lanes), jnp.bfloat16),
            pltpu.VMEM((taps, channels, depth), jnp.bfloat16),
            pltpu.VMEM((channels, channels), jnp.bfloat16),
            pltpu.VMEM(((height + taps - 1) * across, depth), jnp.bfloat16),
            pltpu.VMEM((cells - 2 * across, channels), jnp.float32),
            pltpu.VMEM((stages, 2, across, channels), jnp.bfloat16),
            pltpu.VMEM((stages, cells, channels), jnp.bfloat16),
            pltpu.VMEM((stages, 8, channels), jnp.float32),
            pltpu.VMEM((stages, rows_n, 8, channels), jnp.float32),
            dma((7,)),
            dma((units,)), dma((units,)),
            dma((units,)), dma((units,)),
            dma((units,)), dma((units,)),
            dma((units,)), dma((units,)),
            dma((stages, 2)), dma((stages, 2)),
            dma((stages, rows_n)), dma((stages, rows_n)),
        ],
        compiler_params=pltpu.CompilerParams(
            collective_id=0, has_side_effects=True, vmem_limit_bytes=60 * 1024 * 1024),
    )(
        control.reshape(cells, channels),
        unet_skips.reshape(blocks, cells, channels),
        norm_gains,
        norm_shifts,
        conv,
        zero,
    )
    return out.reshape(blocks, samples, height, across, channels)


def solution(mesh):
    placed = (
        P("batch", "rows", None, None),
        P(None, "batch", "rows", None, None),
        P(),
        P(),
        P(None, None, None, None, "batch"),
        P(None, None, None, "batch"),
    )
    return jax.shard_map(
        functools.partial(on_device, mesh.shape["rows"], mesh.shape["batch"]),
        mesh=mesh,
        in_specs=placed,
        out_specs=P(None, "batch", "rows", None, None),
        check_vma=False,
    )
```

```python
import functools

import jax
import jax.numpy as jnp
from jax import lax
from jax.experimental import pallas as pl
from jax.experimental.pallas import tpu as pltpu
from jax.sharding import PartitionSpec as P

GROUPS = 32
EPSILON = 1e-05
MESH = pl.DeviceIdType.MESH
LOOKAHEAD = 4
DIRECT = (2,)
PLAN = {
    "start": "A0 A1 B0 A2 B1 A3 D0 A4 B2 A5",
    "tap0": "D1 B3",
    "tap1": "B4",
    "tail0": "B5",
    "wait0": "A6 A7 D3 D4",
    "norm1": "D5 A8 B6",
    "half1": "B7 A9",
    "wait1": "A10 D6 B8 A11 D7 B9",
    "norm2": "D8 B10",
    "half2": "D9 B11",
    "wait2": "D10 D11",
}


def transposed(conv_weights, zero_weights):
    blocks, convs, taps, depth, outs = conv_weights.shape
    conv = jnp.transpose(conv_weights, (0, 1, 2, 4, 3)).reshape(blocks * convs * taps, outs, depth)
    return conv, jnp.transpose(zero_weights[:, 0], (0, 2, 1))


def kernel(dims, x_hbm, skip_hbm, gain_hbm, shift_hbm, w_hbm, zw_hbm, out_ref,
           xv, skipv, gainv, shiftv, wv, zwv, group, slabs, wfull, zfull, stk, acc, halo, fields,
           stat_out, stat_in, load,
           z_send, z_recv, a_send, a_recv, b_send, b_recv, d_send, d_recv,
           h_send, h_recv, t_send, t_recv):
    rows_n, batch_n, height, across, channels, outs, taps, members = dims
    units, _, depth = w_hbm.shape
    blocks = zw_hbm.shape[0]
    convs = units // taps
    per_block = convs // blocks
    lanes = slabs.shape[3]
    piece = lanes - depth
    pieces = -(-channels // piece)
    cells = height * across
    zn = batch_n // 2
    r = lax.axis_index("rows")
    b = lax.axis_index("batch")
    z, c = b // 2, b % 2
    bit0, bit1 = r % 2, (r // 2) % 2
    px, py = r + 1 - 2 * bit0, r + 2 - 4 * bit1
    pxy = px + py - r
    mate = b + 1 - 2 * c
    quarter, eighth = lanes // 4, lanes // 8
    g = bit0 * (1 + bit1) + (1 - bit0) * 3 * bit1
    gx = g + 1 - 2 * (g % 2)
    gy = 3 - g
    even = (g + g % 2) % 4
    odd = g + 1 - g % 2

    def part(index):
        return pl.ds(pl.multiple_of(index * quarter, quarter), quarter)

    def first(index):
        return pl.ds(pl.multiple_of(index * quarter, eighth), eighth)

    def second(index):
        return pl.ds(pl.multiple_of(index * quarter + eighth, eighth), eighth)

    def plane(m):
        other, weight = 0, 1
        while weight < zn:
            other = other + ((z // weight + m // weight) % 2) * weight
            weight *= 2
        return other

    def slab(m):
        return plane(m) * 2 + c

    far = list(range(zn - 1, 1, -1))

    def remote(src, dst, send, recv, row, batch):
        return pltpu.make_async_remote_copy(
            src_ref=src, dst_ref=dst, send_sem=send, recv_sem=recv,
            device_id={"rows": row, "batch": batch}, device_id_type=MESH)

    barrier = pltpu.get_barrier_semaphore()
    for j in range(1, zn):
        pl.semaphore_signal(barrier, inc=1, device_id_type=MESH,
                            device_id={"rows": r, "batch": ((z + j) % zn) * 2 + c})
    for j in range(1, rows_n):
        pl.semaphore_signal(barrier, inc=1, device_id_type=MESH,
                            device_id={"rows": (r + j) % rows_n, "batch": b})
    pl.semaphore_signal(barrier, inc=1, device_id_type=MESH, device_id={"rows": r, "batch": mate})

    ahead = min(LOOKAHEAD, units - 1)
    loads = [
        pltpu.make_async_copy(w_hbm.at[pl.ds(0, ahead)], wv.at[pl.ds(0, ahead)], load.at[0]),
        pltpu.make_async_copy(zw_hbm, zwv, load.at[1]),
        pltpu.make_async_copy(x_hbm, xv, load.at[2]),
        pltpu.make_async_copy(w_hbm.at[pl.ds(ahead, units - ahead)], wv.at[pl.ds(ahead, units - ahead)],
                              load.at[3]),
        pltpu.make_async_copy(gain_hbm, gainv, load.at[4]),
        pltpu.make_async_copy(shift_hbm, shiftv, load.at[5]),
        pltpu.make_async_copy(skip_hbm, skipv, load.at[6]),
    ]
    for copy in loads:
        copy.start()

    def pack(u):
        block, p = u // (per_block * taps), u % (per_block * taps)
        slabs[u, b, :, :depth] = wv[u]
        if p < pieces:
            wide = min(piece, channels - p * piece)
            slabs[u, b, :, depth:depth + wide] = zwv[block, :, p * piece:p * piece + wide]

    def z_step(u):
        for m in far:
            here = slabs.at[u, b, :, part(g)]
            remote(here, here, z_send.at[u], z_recv.at[u], r, slab(m)).start()
        for index in (even, odd):
            here = slabs.at[u, b, :, part(index)]
            remote(here, here, z_send.at[u], z_recv.at[u], r, slab(1)).start()

    def own_step(u):
        here = slabs.at[u, b]
        remote(here, here, d_send.at[u], d_recv.at[u], r, mate).start()

    def totals(u):
        return (
            (slabs.at[u, pl.ds(0, zn), :, pl.ds(0, quarter)], z_send, z_recv),
            (slabs.at[u, pl.ds(0, 3 * zn // 2 - 2 if u in DIRECT else zn - 1), :, pl.ds(0, 2 * quarter)],
             a_send, a_recv),
            (slabs.at[u, pl.ds(0, zn - 2), :, pl.ds(0, quarter)], b_send, b_recv),
            (slabs.at[u, pl.ds(0, zn)], d_send, d_recv),
        )

    def arrived(u, stage):
        ref, send, recv = totals(u)[stage]
        remote(ref, ref, send.at[u], recv.at[u], r, mate).wait_recv()

    def a_step(u):
        arrived(u, 0)
        for m in far:
            here = slabs.at[u, slab(m), :, part(g)]
            remote(here, here, a_send.at[u], a_recv.at[u], px, b).start()
            remote(here, here, a_send.at[u], a_recv.at[u], py, b).start()
            if u in DIRECT:
                remote(here, here, a_send.at[u], a_recv.at[u], pxy, b).start()
        here = slabs.at[u, slab(1), :, part(even)]
        remote(here, here, a_send.at[u], a_recv.at[u], px, b).start()
        here = slabs.at[u, slab(1), :, part(odd)]
        remote(here, here, a_send.at[u], a_recv.at[u], py, b).start()

    def b_step(u):
        arrived(u, 1)
        if u in DIRECT:
            for m in far:
                here = slabs.at[u, slab(m)]
                remote(here, here, d_send.at[u], d_recv.at[u], r, mate).start()
        elif far:
            @pl.when(bit0 == bit1)
            def _():
                for m in far:
                    here = slabs.at[u, slab(m), :, first(gy)]
                    remote(here, here, b_send.at[u], b_recv.at[u], px, b).start()
                    here = slabs.at[u, slab(m), :, second(gx)]
                    remote(here, here, b_send.at[u], b_recv.at[u], py, b).start()

            @pl.when(bit0 != bit1)
            def _():
                for m in far:
                    here = slabs.at[u, slab(m), :, part(gx)]
                    remote(here, here, b_send.at[u], b_recv.at[u], py, b).start()
        here = slabs.at[u, slab(1)]
        remote(here, here, d_send.at[u], d_recv.at[u], r, mate).start()

    def d_step(u):
        if u in DIRECT:
            return
        if far:
            arrived(u, 2)
        for m in far:
            here = slabs.at[u, slab(m)]
            remote(here, here, d_send.at[u], d_recv.at[u], r, mate).start()

    stages = {"A": a_step, "B": b_step, "D": d_step}
    done = set()

    def step(kind, u):
        if u >= units or (kind, u) in done:
            return
        for before in "ABD"[:"ABD".index(kind)]:
            step(before, u)
        if kind != "A" and u > 0:
            step(kind, u - 1)
        elif u > 0:
            step("A", u - 1)
        done.add((kind, u))
        stages[kind](u)
        if kind == "A" and u + ahead < units:
            z_step(u + ahead)
            own_step(u + ahead)

    def plan(place):
        for item in PLAN.get(place, "").split():
            step(item[0], int(item[1:]))

    def need(u):
        step("B" if u in DIRECT else "D", u)

    def assemble(u):
        arrived(u, 3)
        for d in range(batch_n):
            wfull[u % taps, d * outs:(d + 1) * outs, :] = slabs[u, d, :, :depth]

    def assemble_zero(block):
        for d in range(batch_n):
            parts = []
            for p in range(pieces):
                wide = min(piece, channels - p * piece)
                parts.append(slabs[block * per_block * taps + p, d, :, depth:depth + wide])
            zfull[d * outs:(d + 1) * outs, :] = jnp.concatenate(parts, axis=1)

    def times(a, w):
        return lax.dot_general(a, w, (((1,), (1,)), ((), ())), preferred_element_type=jnp.float32)

    def halo_copies(s, ref):
        def down():
            return remote(ref.at[pl.ds(cells - across, across)], halo.at[s, 0],
                          h_send.at[s, 0], h_recv.at[s, 0], (r + 1) % rows_n, b)

        def up():
            return remote(ref.at[pl.ds(0, across)], halo.at[s, 1],
                          h_send.at[s, 1], h_recv.at[s, 1], (r + rows_n - 1) % rows_n, b)

        return down, up

    def halo_start(s, ref):
        down, up = halo_copies(s, ref)

        @pl.when(r < rows_n - 1)
        def _():
            down().start()

        @pl.when(r > 0)
        def _():
            up().start()

        return down, up

    sent = []

    def stat_start(s, total, square):
        stat_out[s] = jnp.concatenate([total, square, jnp.zeros((6, channels), jnp.float32)], axis=0)
        for j in range(1, rows_n):
            copy = remote(stat_out.at[s], stat_in.at[s, j], t_send.at[s, j], t_recv.at[s, j],
                          (r + j) % rows_n, b)
            copy.start()
            sent.append(copy)

    col = lax.broadcasted_iota(jnp.int32, (across, channels), 0)

    def normalize(s, ref):
        total = stat_out[s]
        for j in range(1, rows_n):
            here = stat_in.at[s, j]
            remote(here, here, t_send.at[s, j], t_recv.at[s, j], r, mate).wait_recv()
            total = total + stat_in[s, j]
        high = total.astype(jnp.bfloat16).astype(jnp.float32)
        rest = total - high
        middle = rest.astype(jnp.bfloat16).astype(jnp.float32)
        split = jnp.concatenate([high, middle, rest - middle], axis=0).astype(jnp.bfloat16)
        grouped = jnp.dot(split, group[...], preferred_element_type=jnp.float32)
        grouped = (grouped[0:8] + grouped[8:16] + grouped[16:24]) * (1.0 / members)
        mean = grouped[0:1]
        spread = jnp.maximum(grouped[1:2] - mean * mean, 0.0)
        block, half = s // per_block, s % per_block
        scale = lax.rsqrt(spread + EPSILON) * gainv[block, half:half + 1, :]
        bias = shiftv[block, half:half + 1, :] - mean * scale

        def put(at, v, valid):
            y = v.astype(jnp.float32) * scale + bias
            a = y / (1.0 + jnp.exp(-y))
            if valid is not None:
                a = jnp.where(valid, a, 0.0)
            left = jnp.where(col == 0, 0.0, pltpu.roll(a, 1, 0))
            right = jnp.where(col == across - 1, 0.0, pltpu.roll(a, across - 1, 0))
            stk[pl.ds(at, across), :] = jnp.concatenate(
                [left.astype(jnp.bfloat16), a.astype(jnp.bfloat16), right.astype(jnp.bfloat16)], axis=1)

        def body(i, carry):
            at = pl.multiple_of(i * across, across)
            put(pl.multiple_of(at + across, across), ref[pl.ds(at, across), :], None)
            return carry
        lax.fori_loop(0, height, body, 0)

        return put

    def edges(s, put):
        down, up = ends[s]

        @pl.when(r > 0)
        def _():
            down().wait_recv()

        @pl.when(r < rows_n - 1)
        def _():
            up().wait_recv()

        put(0, halo[s, 0], r > 0)
        put((height + 1) * across, halo[s, 1], r < rows_n - 1)

    def keep(s, source, at, value):
        size = value.shape[0]
        if source is not None:
            value = source[at:at + size, :].astype(jnp.float32) + value
        value = value.astype(jnp.bfloat16)
        fields[s, at:at + size, :] = value
        kept = value.astype(jnp.float32)
        return (jnp.sum(kept, axis=0, keepdims=True),
                jnp.sum(kept * kept, axis=0, keepdims=True))

    def convolve(s, source, put):
        units_of = range(s * taps, (s + 1) * taps)
        rows = cells - 2 * across
        if s == 0:
            edges(s, put)
            for t, u in enumerate(units_of):
                need(u)
                assemble(u)
                value = times(stk[t * across:t * across + cells, :], wfull[t])
                if t < taps - 1:
                    acc[...] = value if t == 0 else acc[...] + value
                    plan(f"tap{t}")
            return keep(s, source, 0, acc[...] + value)
        inner = None
        for t, u in enumerate(units_of):
            need(u)
            assemble(u)
            value = times(stk[(t + 1) * across:(t + 1) * across + rows, :], wfull[t])
            inner = value if t == 0 else inner + value
        middle = keep(s, source, across, inner)
        plan(f"half{s}")
        edges(s, put)
        border = None
        for t in range(taps):
            low, high = t * across, (height - 1 + t) * across
            both = jnp.concatenate([stk[low:low + across, :], stk[high:high + across, :]], axis=0)
            value = times(both, wfull[t])
            border = value if t == 0 else border + value
        top = keep(s, source, 0, border[:across])
        bottom = keep(s, source, cells - across, border[across:])
        return middle[0] + top[0] + bottom[0], middle[1] + top[1] + bottom[1]

    def zero_conv(s):
        block = s // per_block
        assemble_zero(block)
        zeroed = times(fields[s], zfull[...])
        out_ref[block] = (skipv[block].astype(jnp.float32) + zeroed).astype(jnp.bfloat16)

    per = channels // GROUPS
    same = (lax.broadcasted_iota(jnp.int32, (channels, channels), 0) // per
            == lax.broadcasted_iota(jnp.int32, (channels, channels), 1) // per)
    group[...] = jnp.where(same, 1.0, 0.0).astype(jnp.bfloat16)

    loads[2].wait()
    whole = xv[...].astype(jnp.float32)
    sums = (jnp.sum(whole, axis=0, keepdims=True), jnp.sum(whole * whole, axis=0, keepdims=True))
    loads[0].wait()
    loads[1].wait()
    for u in range(ahead):
        pack(u)
    pl.semaphore_wait(barrier, zn + rows_n - 1)
    for u in range(ahead):
        z_step(u)
    stat_start(0, *sums)
    ends = [halo_start(0, xv)]
    for u in range(ahead):
        own_step(u)
    loads[3].wait()
    for u in range(ahead, units):
        pack(u)
    for copy in loads[4:]:
        copy.wait()
    put = normalize(0, xv)
    plan("start")
    source = xv
    for s in range(convs):
        if s > 0:
            plan(f"wait{s - 1}")
            put = normalize(s, fields.at[s - 1])
            plan(f"norm{s}")
        last = s % per_block == per_block - 1
        sums = convolve(s, source if last else None, put)
        plan(f"tail{s}")
        if s < convs - 1:
            stat_start(s + 1, *sums)
            ends.append(halo_start(s + 1, fields.at[s]))
        if last:
            source = fields.at[s]
            zero_conv(s)
    need(units - 1)
    for copy in sent:
        copy.wait_send()
    for u in range(units):
        for stage, (ref, send, recv) in enumerate(totals(u)):
            if stage != 2 or far and u not in DIRECT:
                remote(ref, ref, send.at[u], recv.at[u], r, mate).wait_send()
    for down, up in ends:
        @pl.when(r < rows_n - 1)
        def _():
            down().wait_send()

        @pl.when(r > 0)
        def _():
            up().wait_send()


def on_device(rows_n, batch_n, control, unet_skips, norm_gains, norm_shifts, conv_weights, zero_weights):
    blocks, convs, taps, depth, outs = conv_weights.shape
    samples, height, across, channels = control.shape
    lanes = (depth // 512 + 1) * 512
    stages = blocks * convs
    units = stages * taps
    cells = height * across
    per = channels // GROUPS
    conv, zero = transposed(conv_weights, zero_weights)
    members = cells * rows_n * per
    dims = (rows_n, batch_n, height, across, channels, outs, taps, members)
    dma = pltpu.SemaphoreType.DMA
    hbm = pl.BlockSpec(memory_space=pltpu.HBM)
    out = pl.pallas_call(
        functools.partial(kernel, dims),
        out_shape=jax.ShapeDtypeStruct((blocks, cells, channels), jnp.bfloat16),
        in_specs=[hbm] * 6,
        out_specs=pl.BlockSpec(memory_space=pltpu.VMEM),
        scratch_shapes=[
            pltpu.VMEM((cells, channels), jnp.bfloat16),
            pltpu.VMEM((blocks, cells, channels), jnp.bfloat16),
            pltpu.VMEM((blocks, convs, channels), jnp.float32),
            pltpu.VMEM((blocks, convs, channels), jnp.float32),
            pltpu.VMEM((units, outs, depth), jnp.bfloat16),
            pltpu.VMEM((blocks, outs, channels), jnp.bfloat16),
            pltpu.VMEM((channels, channels), jnp.bfloat16),
            pltpu.VMEM((units, batch_n, outs, lanes), jnp.bfloat16),
            pltpu.VMEM((taps, channels, depth), jnp.bfloat16),
            pltpu.VMEM((channels, channels), jnp.bfloat16),
            pltpu.VMEM(((height + taps - 1) * across, depth), jnp.bfloat16),
            pltpu.VMEM((cells, channels), jnp.float32),
            pltpu.VMEM((stages, 2, across, channels), jnp.bfloat16),
            pltpu.VMEM((stages, cells, channels), jnp.bfloat16),
            pltpu.VMEM((stages, 8, channels), jnp.float32),
            pltpu.VMEM((stages, rows_n, 8, channels), jnp.float32),
            dma((7,)),
            dma((units,)), dma((units,)),
            dma((units,)), dma((units,)),
            dma((units,)), dma((units,)),
            dma((units,)), dma((units,)),
            dma((stages, 2)), dma((stages, 2)),
            dma((stages, rows_n)), dma((stages, rows_n)),
        ],
        compiler_params=pltpu.CompilerParams(
            collective_id=0, has_side_effects=True, vmem_limit_bytes=50 * 1024 * 1024),
    )(*(pltpu.with_memory_space_constraint(array, pltpu.HBM) for array in (
        control.reshape(cells, channels),
        unet_skips.reshape(blocks, cells, channels),
        norm_gains,
        norm_shifts,
        conv,
        zero,
    )))
    return out.reshape(blocks, samples, height, across, channels)


def solution(mesh):
    placed = (
        P("batch", "rows", None, None),
        P(None, "batch", "rows", None, None),
        P(),
        P(),
        P(None, None, None, None, "batch"),
        P(None, None, None, "batch"),
    )
    return jax.shard_map(
        functools.partial(on_device, mesh.shape["rows"], mesh.shape["batch"]),
        mesh=mesh,
        in_specs=placed,
        out_specs=P(None, "batch", "rows", None, None),
        check_vma=False,
    )
```

```python
import functools

import jax
import jax.numpy as jnp
from jax import lax
from jax.experimental import pallas as pl
from jax.experimental.pallas import tpu as pltpu
from jax.sharding import PartitionSpec as P

GROUPS = 32
EPSILON = 1e-05
MESH = pl.DeviceIdType.MESH
LOOKAHEAD = 4
DIRECT = (2,)
PLAN = {
    "start": ("A0", "A1", "B0", "A2", "B1", "A3", "D0", "A4"),
    "pre0": ("B2", "A5", "D1"),
    "tap0": ("B3",),
    "tap1": ("B4",),
    "stat0": ("B5",),
    "wait0": ("A6", "D3", "A7", "D4", "A8", "D5", "A9"),
    "half1": ("B6",),
    "stat1": ("B7",),
    "wait1": ("B8", "A10", "D6", "B9", "A11", "D7"),
    "norm2": ("D8",),
    "half2": ("B10", "D9"),
    "wait2": ("B11", "D10"),
    "norm3": ("D11",),
}


def transposed(conv_weights, zero_weights):
    blocks, convs, taps, depth, outs = conv_weights.shape
    conv = jnp.transpose(conv_weights, (0, 1, 2, 4, 3)).reshape(blocks * convs * taps, outs, depth)
    return conv, jnp.transpose(zero_weights[:, 0], (0, 2, 1))


def kernel(dims, x_hbm, skip_hbm, gain_hbm, shift_hbm, w_hbm, zw_hbm, out_ref,
           xv, skipv, gainv, shiftv, wv, zwv, group, slabs, wfull, zfull, stk, acc, halo, fields,
           stat_out, stat_in, load,
           z_send, z_recv, a_send, a_recv, b_send, b_recv, d_send, d_recv,
           h_send, h_recv, t_send, t_recv):
    rows_n, batch_n, height, across, channels, outs, taps, members = dims
    units, _, depth = w_hbm.shape
    blocks = zw_hbm.shape[0]
    convs = units // taps
    per_block = convs // blocks
    lanes = slabs.shape[3]
    piece = lanes - depth
    pieces = -(-channels // piece)
    cells = height * across
    zn = batch_n // 2
    r = lax.axis_index("rows")
    b = lax.axis_index("batch")
    z, c = b // 2, b % 2
    bit0, bit1 = r % 2, (r // 2) % 2
    px, py = r + 1 - 2 * bit0, r + 2 - 4 * bit1
    pxy = px + py - r
    mate = b + 1 - 2 * c
    quarter, eighth = lanes // 4, lanes // 8
    g = bit0 * (1 + bit1) + (1 - bit0) * 3 * bit1
    gx = g + 1 - 2 * (g % 2)
    gy = 3 - g
    even = (g + g % 2) % 4
    odd = g + 1 - g % 2

    def part(index):
        return pl.ds(pl.multiple_of(index * quarter, quarter), quarter)

    def first(index):
        return pl.ds(pl.multiple_of(index * quarter, eighth), eighth)

    def second(index):
        return pl.ds(pl.multiple_of(index * quarter + eighth, eighth), eighth)

    def plane(m):
        other, weight = 0, 1
        while weight < zn:
            other = other + ((z // weight + m // weight) % 2) * weight
            weight *= 2
        return other

    def slab(m):
        return plane(m) * 2 + c

    far = list(range(zn - 1, 1, -1))

    def remote(src, dst, send, recv, row, batch):
        return pltpu.make_async_remote_copy(
            src_ref=src, dst_ref=dst, send_sem=send, recv_sem=recv,
            device_id={"rows": row, "batch": batch}, device_id_type=MESH)

    barrier = pltpu.get_barrier_semaphore()
    for j in range(1, zn):
        pl.semaphore_signal(barrier, inc=1, device_id_type=MESH,
                            device_id={"rows": r, "batch": ((z + j) % zn) * 2 + c})
    for j in range(1, rows_n):
        pl.semaphore_signal(barrier, inc=1, device_id_type=MESH,
                            device_id={"rows": (r + j) % rows_n, "batch": b})
    pl.semaphore_signal(barrier, inc=1, device_id_type=MESH, device_id={"rows": r, "batch": mate})

    ahead = min(LOOKAHEAD, units - 1)
    loads = [
        pltpu.make_async_copy(w_hbm.at[pl.ds(0, ahead)], wv.at[pl.ds(0, ahead)], load.at[0]),
        pltpu.make_async_copy(zw_hbm, zwv, load.at[1]),
        pltpu.make_async_copy(x_hbm, xv, load.at[2]),
        pltpu.make_async_copy(w_hbm.at[pl.ds(ahead, units - ahead)], wv.at[pl.ds(ahead, units - ahead)],
                              load.at[3]),
        pltpu.make_async_copy(gain_hbm, gainv, load.at[4]),
        pltpu.make_async_copy(shift_hbm, shiftv, load.at[5]),
        pltpu.make_async_copy(skip_hbm, skipv, load.at[6]),
    ]
    for copy in loads:
        copy.start()

    def pack(u):
        block, p = u // (per_block * taps), u % (per_block * taps)
        slabs[u, b, :, :depth] = wv[u]
        if p < pieces:
            wide = min(piece, channels - p * piece)
            slabs[u, b, :, depth:depth + wide] = zwv[block, :, p * piece:p * piece + wide]

    def z_step(u):
        for m in far:
            here = slabs.at[u, b, :, part(g)]
            remote(here, here, z_send.at[u], z_recv.at[u], r, slab(m)).start()
        for index in (even, odd):
            here = slabs.at[u, b, :, part(index)]
            remote(here, here, z_send.at[u], z_recv.at[u], r, slab(1)).start()

    def own_step(u):
        here = slabs.at[u, b]
        remote(here, here, d_send.at[u], d_recv.at[u], r, mate).start()

    def totals(u):
        return (
            (slabs.at[u, pl.ds(0, zn), :, pl.ds(0, quarter)], z_send, z_recv),
            (slabs.at[u, pl.ds(0, 3 * zn // 2 - 2 if u in DIRECT else zn - 1), :, pl.ds(0, 2 * quarter)],
             a_send, a_recv),
            (slabs.at[u, pl.ds(0, zn - 2), :, pl.ds(0, quarter)], b_send, b_recv),
            (slabs.at[u, pl.ds(0, zn)], d_send, d_recv),
        )

    def arrived(u, stage):
        ref, send, recv = totals(u)[stage]
        remote(ref, ref, send.at[u], recv.at[u], r, mate).wait_recv()

    def a_step(u):
        arrived(u, 0)
        for m in far:
            here = slabs.at[u, slab(m), :, part(g)]
            remote(here, here, a_send.at[u], a_recv.at[u], px, b).start()
            remote(here, here, a_send.at[u], a_recv.at[u], py, b).start()
            if u in DIRECT:
                remote(here, here, a_send.at[u], a_recv.at[u], pxy, b).start()
        here = slabs.at[u, slab(1), :, part(even)]
        remote(here, here, a_send.at[u], a_recv.at[u], px, b).start()
        here = slabs.at[u, slab(1), :, part(odd)]
        remote(here, here, a_send.at[u], a_recv.at[u], py, b).start()

    def b_step(u):
        arrived(u, 1)
        if u in DIRECT:
            for m in far:
                here = slabs.at[u, slab(m)]
                remote(here, here, d_send.at[u], d_recv.at[u], r, mate).start()
        elif far:
            @pl.when(bit0 == bit1)
            def _():
                for m in far:
                    here = slabs.at[u, slab(m), :, first(gy)]
                    remote(here, here, b_send.at[u], b_recv.at[u], px, b).start()
                    here = slabs.at[u, slab(m), :, second(gx)]
                    remote(here, here, b_send.at[u], b_recv.at[u], py, b).start()

            @pl.when(bit0 != bit1)
            def _():
                for m in far:
                    here = slabs.at[u, slab(m), :, part(gx)]
                    remote(here, here, b_send.at[u], b_recv.at[u], py, b).start()
        here = slabs.at[u, slab(1)]
        remote(here, here, d_send.at[u], d_recv.at[u], r, mate).start()

    def d_step(u):
        if u in DIRECT:
            return
        if far:
            arrived(u, 2)
        for m in far:
            here = slabs.at[u, slab(m)]
            remote(here, here, d_send.at[u], d_recv.at[u], r, mate).start()

    stages = {"A": a_step, "B": b_step, "D": d_step}
    done = set()

    def step(kind, u):
        if u >= units or (kind, u) in done:
            return
        for before in "ABD"[:"ABD".index(kind)]:
            step(before, u)
        if kind != "A" and u > 0:
            step(kind, u - 1)
        elif u > 0:
            step("A", u - 1)
        done.add((kind, u))
        stages[kind](u)
        if kind == "A" and u + ahead < units:
            z_step(u + ahead)
            own_step(u + ahead)

    def plan(place):
        for item in PLAN.get(place, ()):
            step(item[0], int(item[1:]))

    def need(u):
        step("B" if u in DIRECT else "D", u)

    def assemble(u):
        arrived(u, 3)
        for d in range(batch_n):
            wfull[u % taps, d * outs:(d + 1) * outs, :] = slabs[u, d, :, :depth]

    def assemble_zero(block):
        for d in range(batch_n):
            parts = []
            for p in range(pieces):
                wide = min(piece, channels - p * piece)
                parts.append(slabs[block * per_block * taps + p, d, :, depth:depth + wide])
            zfull[d * outs:(d + 1) * outs, :] = jnp.concatenate(parts, axis=1)

    def times(a, w):
        return lax.dot_general(a, w, (((1,), (1,)), ((), ())), preferred_element_type=jnp.float32)

    def halo_copies(s, ref):
        def down():
            return remote(ref.at[pl.ds(cells - across, across)], halo.at[s, 0],
                          h_send.at[s, 0], h_recv.at[s, 0], (r + 1) % rows_n, b)

        def up():
            return remote(ref.at[pl.ds(0, across)], halo.at[s, 1],
                          h_send.at[s, 1], h_recv.at[s, 1], (r + rows_n - 1) % rows_n, b)

        return down, up

    def halo_start(s, ref):
        down, up = halo_copies(s, ref)

        @pl.when(r < rows_n - 1)
        def _():
            down().start()

        @pl.when(r > 0)
        def _():
            up().start()

        return down, up

    sent = []

    def stat_start(s, total, square):
        stat_out[s] = jnp.concatenate([total, square, jnp.zeros((6, channels), jnp.float32)], axis=0)
        for j in range(1, rows_n):
            copy = remote(stat_out.at[s], stat_in.at[s, j], t_send.at[s, j], t_recv.at[s, j],
                          (r + j) % rows_n, b)
            copy.start()
            sent.append(copy)

    col = lax.broadcasted_iota(jnp.int32, (across, channels), 0)

    def normalize(s, ref):
        total = stat_out[s]
        for j in range(1, rows_n):
            here = stat_in.at[s, j]
            remote(here, here, t_send.at[s, j], t_recv.at[s, j], r, mate).wait_recv()
            total = total + stat_in[s, j]
        high = total.astype(jnp.bfloat16).astype(jnp.float32)
        rest = total - high
        middle = rest.astype(jnp.bfloat16).astype(jnp.float32)
        split = jnp.concatenate([high, middle, rest - middle], axis=0).astype(jnp.bfloat16)
        grouped = jnp.dot(split, group[...], preferred_element_type=jnp.float32)
        grouped = (grouped[0:8] + grouped[8:16] + grouped[16:24]) * (1.0 / members)
        mean = grouped[0:1]
        spread = jnp.maximum(grouped[1:2] - mean * mean, 0.0)
        block, half = s // per_block, s % per_block
        scale = lax.rsqrt(spread + EPSILON) * gainv[block, half:half + 1, :]
        bias = shiftv[block, half:half + 1, :] - mean * scale

        def put(at, v, valid):
            y = v.astype(jnp.float32) * scale + bias
            a = y / (1.0 + jnp.exp(-y))
            if valid is not None:
                a = jnp.where(valid, a, 0.0)
            left = jnp.where(col == 0, 0.0, pltpu.roll(a, 1, 0))
            right = jnp.where(col == across - 1, 0.0, pltpu.roll(a, across - 1, 0))
            stk[pl.ds(at, across), :] = jnp.concatenate(
                [left.astype(jnp.bfloat16), a.astype(jnp.bfloat16), right.astype(jnp.bfloat16)], axis=1)

        def body(i, carry):
            at = pl.multiple_of(i * across, across)
            put(pl.multiple_of(at + across, across), ref[pl.ds(at, across), :], None)
            return carry
        lax.fori_loop(0, height, body, 0)

        return put

    def edges(s, put):
        down, up = ends[s]

        @pl.when(r > 0)
        def _():
            down().wait_recv()

        @pl.when(r < rows_n - 1)
        def _():
            up().wait_recv()

        put(0, halo[s, 0], r > 0)
        put((height + 1) * across, halo[s, 1], r < rows_n - 1)

    def keep(s, source, at, value):
        size = value.shape[0]
        if source is not None:
            value = source[at:at + size, :].astype(jnp.float32) + value
        value = value.astype(jnp.bfloat16)
        fields[s, at:at + size, :] = value
        kept = value.astype(jnp.float32)
        return (jnp.sum(kept, axis=0, keepdims=True),
                jnp.sum(kept * kept, axis=0, keepdims=True))

    def convolve(s, source, put):
        units_of = range(s * taps, (s + 1) * taps)
        rows = cells - 2 * across
        if s == 0:
            edges(s, put)
            for t, u in enumerate(units_of):
                need(u)
                assemble(u)
                value = times(stk[t * across:t * across + cells, :], wfull[t])
                if t < taps - 1:
                    acc[...] = value if t == 0 else acc[...] + value
                    if t == 0:
                        plan("pre0")
                    plan(f"tap{t}")
            return keep(s, source, 0, acc[...] + value)
        inner = None
        for t, u in enumerate(units_of):
            need(u)
            assemble(u)
            value = times(stk[(t + 1) * across:(t + 1) * across + rows, :], wfull[t])
            inner = value if t == 0 else inner + value
        middle = keep(s, source, across, inner)
        plan(f"half{s}")
        edges(s, put)
        border = None
        for t in range(taps):
            low, high = t * across, (height - 1 + t) * across
            both = jnp.concatenate([stk[low:low + across, :], stk[high:high + across, :]], axis=0)
            value = times(both, wfull[t])
            border = value if t == 0 else border + value
        top = keep(s, source, 0, border[:across])
        bottom = keep(s, source, cells - across, border[across:])
        return middle[0] + top[0] + bottom[0], middle[1] + top[1] + bottom[1]

    def zero_conv(s):
        block = s // per_block
        assemble_zero(block)
        zeroed = times(fields[s], zfull[...])
        out_ref[block] = (skipv[block].astype(jnp.float32) + zeroed).astype(jnp.bfloat16)

    per = channels // GROUPS
    same = (lax.broadcasted_iota(jnp.int32, (channels, channels), 0) // per
            == lax.broadcasted_iota(jnp.int32, (channels, channels), 1) // per)
    group[...] = jnp.where(same, 1.0, 0.0).astype(jnp.bfloat16)

    loads[2].wait()
    whole = xv[...].astype(jnp.float32)
    sums = (jnp.sum(whole, axis=0, keepdims=True), jnp.sum(whole * whole, axis=0, keepdims=True))
    loads[0].wait()
    loads[1].wait()
    for u in range(ahead):
        pack(u)
    pl.semaphore_wait(barrier, zn + rows_n - 1)
    for u in range(ahead):
        z_step(u)
    stat_start(0, *sums)
    ends = [halo_start(0, xv)]
    for u in range(ahead):
        own_step(u)
    loads[3].wait()
    for u in range(ahead, units):
        pack(u)
    for copy in loads[4:]:
        copy.wait()
    put = normalize(0, xv)
    plan("start")
    source = xv
    for s in range(convs):
        if s > 0:
            plan(f"wait{s - 1}")
            put = normalize(s, fields.at[s - 1])
            plan(f"norm{s}")
        last = s % per_block == per_block - 1
        sums = convolve(s, source if last else None, put)
        if s < convs - 1:
            stat_start(s + 1, *sums)
            plan(f"stat{s}")
            ends.append(halo_start(s + 1, fields.at[s]))
        if last:
            source = fields.at[s]
            zero_conv(s)
    need(units - 1)
    for copy in sent:
        copy.wait_send()
    for u in range(units):
        for stage, (ref, send, recv) in enumerate(totals(u)):
            if stage != 2 or far and u not in DIRECT:
                remote(ref, ref, send.at[u], recv.at[u], r, mate).wait_send()
    for down, up in ends:
        @pl.when(r < rows_n - 1)
        def _():
            down().wait_send()

        @pl.when(r > 0)
        def _():
            up().wait_send()


def on_device(rows_n, batch_n, control, unet_skips, norm_gains, norm_shifts, conv_weights, zero_weights):
    blocks, convs, taps, depth, outs = conv_weights.shape
    samples, height, across, channels = control.shape
    lanes = (depth // 512 + 1) * 512
    stages = blocks * convs
    units = stages * taps
    cells = height * across
    per = channels // GROUPS
    conv, zero = transposed(conv_weights, zero_weights)
    members = cells * rows_n * per
    dims = (rows_n, batch_n, height, across, channels, outs, taps, members)
    dma = pltpu.SemaphoreType.DMA
    hbm = pl.BlockSpec(memory_space=pltpu.HBM)
    out = pl.pallas_call(
        functools.partial(kernel, dims),
        out_shape=jax.ShapeDtypeStruct((blocks, cells, channels), jnp.bfloat16),
        in_specs=[hbm] * 6,
        out_specs=pl.BlockSpec(memory_space=pltpu.VMEM),
        scratch_shapes=[
            pltpu.VMEM((cells, channels), jnp.bfloat16),
            pltpu.VMEM((blocks, cells, channels), jnp.bfloat16),
            pltpu.VMEM((blocks, convs, channels), jnp.float32),
            pltpu.VMEM((blocks, convs, channels), jnp.float32),
            pltpu.VMEM((units, outs, depth), jnp.bfloat16),
            pltpu.VMEM((blocks, outs, channels), jnp.bfloat16),
            pltpu.VMEM((channels, channels), jnp.bfloat16),
            pltpu.VMEM((units, batch_n, outs, lanes), jnp.bfloat16),
            pltpu.VMEM((taps, channels, depth), jnp.bfloat16),
            pltpu.VMEM((channels, channels), jnp.bfloat16),
            pltpu.VMEM(((height + taps - 1) * across, depth), jnp.bfloat16),
            pltpu.VMEM((cells, channels), jnp.float32),
            pltpu.VMEM((stages, 2, across, channels), jnp.bfloat16),
            pltpu.VMEM((stages, cells, channels), jnp.bfloat16),
            pltpu.VMEM((stages, 8, channels), jnp.float32),
            pltpu.VMEM((stages, rows_n, 8, channels), jnp.float32),
            dma((7,)),
            dma((units,)), dma((units,)),
            dma((units,)), dma((units,)),
            dma((units,)), dma((units,)),
            dma((units,)), dma((units,)),
            dma((stages, 2)), dma((stages, 2)),
            dma((stages, rows_n)), dma((stages, rows_n)),
        ],
        compiler_params=pltpu.CompilerParams(
            collective_id=0, has_side_effects=True, vmem_limit_bytes=50 * 1024 * 1024),
    )(*(pltpu.with_memory_space_constraint(array, pltpu.HBM) for array in (
        control.reshape(cells, channels),
        unet_skips.reshape(blocks, cells, channels),
        norm_gains,
        norm_shifts,
        conv,
        zero,
    )))
    return out.reshape(blocks, samples, height, across, channels)


def solution(mesh):
    placed = (
        P("batch", "rows", None, None),
        P(None, "batch", "rows", None, None),
        P(),
        P(),
        P(None, None, None, None, "batch"),
        P(None, None, None, "batch"),
    )
    return jax.shard_map(
        functools.partial(on_device, mesh.shape["rows"], mesh.shape["batch"]),
        mesh=mesh,
        in_specs=placed,
        out_specs=P(None, "batch", "rows", None, None),
        check_vma=False,
    )
```

```python
import functools

import jax
import jax.numpy as jnp
from jax import lax
from jax.experimental import pallas as pl
from jax.experimental.pallas import tpu as pltpu
from jax.sharding import PartitionSpec as P

GROUPS = 32
EPSILON = 1e-05
MESH = pl.DeviceIdType.MESH
LOOKAHEAD = 4
DIRECT = (2,)
PLAN = {
    "start": ("A0", "A1", "B0", "A2", "B1", "A3", "D0", "A4"),
    "half0": ("B2", "A5", "D1", "B3"),
    "tap1": ("B4",),
    "stat0": ("B5",),
    "wait0": ("A6", "D3", "A7", "D4", "A8", "D5"),
    "edge1": ("B6",),
    "stat1": ("B7",),
    "wait1": ("B8", "A9", "D6", "A10", "D7", "A11"),
    "norm2": ("D8",),
    "edge2": ("B9",),
    "stat2": ("B10",),
    "wait2": ("B11", "D9", "D10"),
    "norm3": ("D11",),
}


def transposed(conv_weights, zero_weights):
    blocks, convs, taps, depth, outs = conv_weights.shape
    conv = jnp.transpose(conv_weights, (0, 1, 2, 4, 3)).reshape(blocks * convs * taps, outs, depth)
    return conv, jnp.transpose(zero_weights[:, 0], (0, 2, 1))


def kernel(dims, x_hbm, skip_hbm, gain_hbm, shift_hbm, w_hbm, zw_hbm, out_ref,
           xv, skipv, gainv, shiftv, wv, zwv, group, slabs, wfull, zfull, stk, acc, halo, fields,
           stat_out, stat_in, load,
           z_send, z_recv, a_send, a_recv, b_send, b_recv, d_send, d_recv,
           h_send, h_recv, t_send, t_recv):
    rows_n, batch_n, height, across, channels, outs, taps, members = dims
    units, _, depth = w_hbm.shape
    blocks = zw_hbm.shape[0]
    convs = units // taps
    per_block = convs // blocks
    lanes = slabs.shape[3]
    piece = lanes - depth
    pieces = -(-channels // piece)
    cells = height * across
    zn = batch_n // 2
    r = lax.axis_index("rows")
    b = lax.axis_index("batch")
    z, c = b // 2, b % 2
    bit0, bit1 = r % 2, (r // 2) % 2
    px, py = r + 1 - 2 * bit0, r + 2 - 4 * bit1
    pxy = px + py - r
    mate = b + 1 - 2 * c
    quarter, eighth = lanes // 4, lanes // 8
    g = bit0 * (1 + bit1) + (1 - bit0) * 3 * bit1
    gx = g + 1 - 2 * (g % 2)
    gy = 3 - g
    even = (g + g % 2) % 4
    odd = g + 1 - g % 2

    def part(index):
        return pl.ds(pl.multiple_of(index * quarter, quarter), quarter)

    def first(index):
        return pl.ds(pl.multiple_of(index * quarter, eighth), eighth)

    def second(index):
        return pl.ds(pl.multiple_of(index * quarter + eighth, eighth), eighth)

    def plane(m):
        other, weight = 0, 1
        while weight < zn:
            other = other + ((z // weight + m // weight) % 2) * weight
            weight *= 2
        return other

    def slab(m):
        return plane(m) * 2 + c

    far = list(range(zn - 1, 1, -1))
    order = [taps // 2] + [t for t in range(taps) if t != taps // 2]

    def remote(src, dst, send, recv, row, batch):
        return pltpu.make_async_remote_copy(
            src_ref=src, dst_ref=dst, send_sem=send, recv_sem=recv,
            device_id={"rows": row, "batch": batch}, device_id_type=MESH)

    barrier = pltpu.get_barrier_semaphore()
    for j in range(1, zn):
        pl.semaphore_signal(barrier, inc=1, device_id_type=MESH,
                            device_id={"rows": r, "batch": ((z + j) % zn) * 2 + c})
    for j in range(1, rows_n):
        pl.semaphore_signal(barrier, inc=1, device_id_type=MESH,
                            device_id={"rows": (r + j) % rows_n, "batch": b})
    pl.semaphore_signal(barrier, inc=1, device_id_type=MESH, device_id={"rows": r, "batch": mate})

    ahead = min(LOOKAHEAD, units - 1)
    early = -(-ahead // taps) * taps
    loads = [
        pltpu.make_async_copy(w_hbm.at[pl.ds(0, early)], wv.at[pl.ds(0, early)], load.at[0]),
        pltpu.make_async_copy(zw_hbm, zwv, load.at[1]),
        pltpu.make_async_copy(x_hbm, xv, load.at[2]),
        pltpu.make_async_copy(w_hbm.at[pl.ds(early, units - early)], wv.at[pl.ds(early, units - early)],
                              load.at[3]),
        pltpu.make_async_copy(gain_hbm, gainv, load.at[4]),
        pltpu.make_async_copy(shift_hbm, shiftv, load.at[5]),
        pltpu.make_async_copy(skip_hbm, skipv, load.at[6]),
    ]
    for copy in loads:
        copy.start()

    def pack(u):
        block, p = u // (per_block * taps), u % (per_block * taps)
        slabs[u, b, :, :depth] = wv[u // taps * taps + order[u % taps]]
        if p < pieces:
            wide = min(piece, channels - p * piece)
            slabs[u, b, :, depth:depth + wide] = zwv[block, :, p * piece:p * piece + wide]

    def z_step(u):
        for m in far:
            here = slabs.at[u, b, :, part(g)]
            remote(here, here, z_send.at[0], z_recv.at[u], r, slab(m)).start()
        for index in (even, odd):
            here = slabs.at[u, b, :, part(index)]
            remote(here, here, z_send.at[0], z_recv.at[u], r, slab(1)).start()

    def own_step(u):
        here = slabs.at[u, b]
        remote(here, here, d_send.at[0], d_recv.at[u], r, mate).start()

    def totals(u):
        return (
            (slabs.at[u, pl.ds(0, zn), :, pl.ds(0, quarter)], z_send, z_recv),
            (slabs.at[u, pl.ds(0, 3 * zn // 2 - 2 if u in DIRECT else zn - 1), :, pl.ds(0, 2 * quarter)],
             a_send, a_recv),
            (slabs.at[u, pl.ds(0, zn - 2), :, pl.ds(0, quarter)], b_send, b_recv),
            (slabs.at[u, pl.ds(0, zn)], d_send, d_recv),
        )

    def arrived(u, stage):
        ref, send, recv = totals(u)[stage]
        remote(ref, ref, send.at[0], recv.at[u], r, mate).wait_recv()

    def a_step(u):
        arrived(u, 0)
        for m in far:
            here = slabs.at[u, slab(m), :, part(g)]
            remote(here, here, a_send.at[0], a_recv.at[u], px, b).start()
            remote(here, here, a_send.at[0], a_recv.at[u], py, b).start()
            if u in DIRECT:
                remote(here, here, a_send.at[1], a_recv.at[u], pxy, b).start()
        here = slabs.at[u, slab(1), :, part(even)]
        remote(here, here, a_send.at[0], a_recv.at[u], px, b).start()
        here = slabs.at[u, slab(1), :, part(odd)]
        remote(here, here, a_send.at[0], a_recv.at[u], py, b).start()

    def b_step(u):
        arrived(u, 1)
        if u in DIRECT:
            for m in far:
                here = slabs.at[u, slab(m)]
                remote(here, here, d_send.at[0], d_recv.at[u], r, mate).start()
        elif far:
            @pl.when(bit0 == bit1)
            def _():
                for m in far:
                    here = slabs.at[u, slab(m), :, first(gy)]
                    remote(here, here, b_send.at[0], b_recv.at[u], px, b).start()
                    here = slabs.at[u, slab(m), :, second(gx)]
                    remote(here, here, b_send.at[0], b_recv.at[u], py, b).start()

            @pl.when(bit0 != bit1)
            def _():
                for m in far:
                    here = slabs.at[u, slab(m), :, part(gx)]
                    remote(here, here, b_send.at[0], b_recv.at[u], py, b).start()
        here = slabs.at[u, slab(1)]
        remote(here, here, d_send.at[0], d_recv.at[u], r, mate).start()

    def d_step(u):
        if u in DIRECT:
            return
        if far:
            arrived(u, 2)
        for m in far:
            here = slabs.at[u, slab(m)]
            remote(here, here, d_send.at[0], d_recv.at[u], r, mate).start()

    stages = {"A": a_step, "B": b_step, "D": d_step}
    done = set()

    def step(kind, u):
        if u >= units or (kind, u) in done:
            return
        for before in "ABD"[:"ABD".index(kind)]:
            step(before, u)
        if kind != "A" and u > 0:
            step(kind, u - 1)
        elif u > 0:
            step("A", u - 1)
        done.add((kind, u))
        stages[kind](u)
        if kind == "A" and u + ahead < units:
            z_step(u + ahead)
            own_step(u + ahead)

    def plan(place):
        for item in PLAN.get(place, ()):
            step(item[0], int(item[1:]))

    def drain():
        direct = len(DIRECT)
        plain = units - direct
        sends = [
            (slabs.at[:, pl.ds(0, zn), :, pl.ds(0, quarter)], z_send.at[0]),
            (slabs.at[:, pl.ds(0, zn - 1), :, pl.ds(0, 2 * quarter)], a_send.at[0]),
            (slabs.at[:, pl.ds(0, zn)], d_send.at[0]),
            (stat_in.at[pl.ds(1, convs - 1), pl.ds(1, rows_n - 1)], t_send.at[1]),
            (stat_in.at[0, pl.ds(1, rows_n - 1)], t_send.at[0]),
        ]
        if far:
            sends += [
                (slabs.at[pl.ds(0, direct), pl.ds(0, zn - 2), :, pl.ds(0, quarter)], a_send.at[1]),
                (slabs.at[pl.ds(0, plain), pl.ds(0, zn - 2), :, pl.ds(0, quarter)], b_send.at[0]),
            ]
        for ref, send in sends:
            remote(ref, ref, send, t_recv.at[0], r, mate).wait_send()
        for down, up in ends:
            pl.when(r < rows_n - 1)(lambda: down().wait_send())
            pl.when(r > 0)(lambda: up().wait_send())

    def need(u):
        step("B" if u in DIRECT else "D", u)

    def assemble(u):
        arrived(u, 3)
        for d in range(batch_n):
            wfull[order[u % taps], d * outs:(d + 1) * outs, :] = slabs[u, d, :, :depth]

    def assemble_zero(block):
        for d in range(batch_n):
            parts = []
            for p in range(pieces):
                wide = min(piece, channels - p * piece)
                parts.append(slabs[block * per_block * taps + p, d, :, depth:depth + wide])
            zfull[d * outs:(d + 1) * outs, :] = jnp.concatenate(parts, axis=1)

    def times(a, w):
        return lax.dot_general(a, w, (((1,), (1,)), ((), ())), preferred_element_type=jnp.float32)

    def halo_copies(s, ref):
        def down():
            return remote(ref.at[pl.ds(cells - across, across)], halo.at[s, 0],
                          h_send.at[s, 0], h_recv.at[s, 0], (r + 1) % rows_n, b)

        def up():
            return remote(ref.at[pl.ds(0, across)], halo.at[s, 1],
                          h_send.at[s, 1], h_recv.at[s, 1], (r + rows_n - 1) % rows_n, b)

        return down, up

    def halo_start(s, ref):
        down, up = halo_copies(s, ref)

        @pl.when(r < rows_n - 1)
        def _():
            down().start()

        @pl.when(r > 0)
        def _():
            up().start()

        return down, up

    def stat_start(s, total, square):
        stat_out[s] = jnp.concatenate([total, square, jnp.zeros((6, channels), jnp.float32)], axis=0)
        for j in range(1, rows_n):
            remote(stat_out.at[s], stat_in.at[s, j], t_send.at[min(s, 1)], t_recv.at[s],
                   (r + j) % rows_n, b).start()

    col = lax.broadcasted_iota(jnp.int32, (across, channels), 0)

    def normalize(s, ref):
        total = stat_out[s]
        here = stat_in.at[s, pl.ds(1, rows_n - 1)]
        remote(here, here, t_send.at[0], t_recv.at[s], r, mate).wait_recv()
        for j in range(1, rows_n):
            total = total + stat_in[s, j]
        high = total.astype(jnp.bfloat16).astype(jnp.float32)
        rest = total - high
        middle = rest.astype(jnp.bfloat16).astype(jnp.float32)
        split = jnp.concatenate([high, middle, rest - middle], axis=0).astype(jnp.bfloat16)
        grouped = jnp.dot(split, group[...], preferred_element_type=jnp.float32)
        grouped = (grouped[0:8] + grouped[8:16] + grouped[16:24]) * (1.0 / members)
        mean = grouped[0:1]
        spread = jnp.maximum(grouped[1:2] - mean * mean, 0.0)
        block, half = s // per_block, s % per_block
        scale = lax.rsqrt(spread + EPSILON) * gainv[block, half:half + 1, :]
        bias = shiftv[block, half:half + 1, :] - mean * scale

        def put(at, v, valid):
            y = v.astype(jnp.float32) * scale + bias
            half = 0.5 * y
            a = half + half * jnp.tanh(half)
            if valid is not None:
                a = jnp.where(valid, a, 0.0)
            left = jnp.where(col == 0, 0.0, pltpu.roll(a, 1, 0))
            right = jnp.where(col == across - 1, 0.0, pltpu.roll(a, across - 1, 0))
            stk[pl.ds(at, across), :] = jnp.concatenate(
                [left.astype(jnp.bfloat16), a.astype(jnp.bfloat16), right.astype(jnp.bfloat16)], axis=1)

        def body(i, carry):
            at = pl.multiple_of(i * across, across)
            put(pl.multiple_of(at + across, across), ref[pl.ds(at, across), :], None)
            return carry
        lax.fori_loop(0, height, body, 0)

        return put

    def edges(s, put):
        down, up = ends[s]

        @pl.when(r > 0)
        def _():
            down().wait_recv()

        @pl.when(r < rows_n - 1)
        def _():
            up().wait_recv()

        put(0, halo[s, 0], r > 0)
        put((height + 1) * across, halo[s, 1], r < rows_n - 1)

    def keep(s, source, at, value):
        size = value.shape[0]
        if source is not None:
            value = source[at:at + size, :].astype(jnp.float32) + value
        value = value.astype(jnp.bfloat16)
        fields[s, at:at + size, :] = value
        kept = value.astype(jnp.float32)
        return (jnp.sum(kept, axis=0, keepdims=True),
                jnp.sum(kept * kept, axis=0, keepdims=True))

    def convolve(s, source, put):
        last = s % per_block == per_block - 1
        total = None
        for i in range(taps):
            t = order[i]
            if i == 0 or s == 0:
                need(s * taps + i)
                assemble(s * taps + i)
            elif i == 1:
                for j in range(1, taps):
                    need(s * taps + j)
                    assemble(s * taps + j)
                if last:
                    assemble_zero(s // per_block)
                plan(f"edge{s}")
            value = times(stk[t * across:t * across + cells, :], wfull[t])
            if i == 0 or s == 0 and i < taps - 1:
                acc[...] = value if i == 0 else acc[...] + value
            else:
                total = value if total is None else total + value
            if i == 0:
                plan(f"half{s}")
                edges(s, put)
            if s == 0:
                plan(f"tap{i}")
        return keep(s, source, 0, acc[...] + total)

    def zero_conv(s):
        block = s // per_block
        zeroed = times(fields[s], zfull[...])
        out_ref[block] = (skipv[block].astype(jnp.float32) + zeroed).astype(jnp.bfloat16)

    per = channels // GROUPS
    same = (lax.broadcasted_iota(jnp.int32, (channels, channels), 0) // per
            == lax.broadcasted_iota(jnp.int32, (channels, channels), 1) // per)
    group[...] = jnp.where(same, 1.0, 0.0).astype(jnp.bfloat16)

    loads[2].wait()
    whole = xv[...].astype(jnp.float32)
    sums = (jnp.sum(whole, axis=0, keepdims=True), jnp.sum(whole * whole, axis=0, keepdims=True))
    loads[0].wait()
    loads[1].wait()
    for u in range(ahead):
        pack(u)
    pl.semaphore_wait(barrier, zn + rows_n - 1)
    for u in range(ahead):
        z_step(u)
    stat_start(0, *sums)
    ends = [halo_start(0, xv)]
    for u in range(ahead):
        own_step(u)
    loads[3].wait()
    for u in range(ahead, units):
        pack(u)
    for copy in loads[4:]:
        copy.wait()
    put = normalize(0, xv)
    plan("start")
    source = xv
    for s in range(convs):
        if s > 0:
            plan(f"wait{s - 1}")
            put = normalize(s, fields.at[s - 1])
            plan(f"norm{s}")
        last = s % per_block == per_block - 1
        sums = convolve(s, source if last else None, put)
        if s < convs - 1:
            stat_start(s + 1, *sums)
            plan(f"stat{s}")
            ends.append(halo_start(s + 1, fields.at[s]))
        if last:
            source = fields.at[s]
            zero_conv(s)
    need(units - 1)
    drain()


def on_device(rows_n, batch_n, control, unet_skips, norm_gains, norm_shifts, conv_weights, zero_weights):
    blocks, convs, taps, depth, outs = conv_weights.shape
    samples, height, across, channels = control.shape
    lanes = (depth // 512 + 1) * 512
    stages = blocks * convs
    units = stages * taps
    cells = height * across
    per = channels // GROUPS
    conv, zero = transposed(conv_weights, zero_weights)
    members = cells * rows_n * per
    dims = (rows_n, batch_n, height, across, channels, outs, taps, members)
    dma = pltpu.SemaphoreType.DMA
    hbm = pl.BlockSpec(memory_space=pltpu.HBM)
    out = pl.pallas_call(
        functools.partial(kernel, dims),
        out_shape=jax.ShapeDtypeStruct((blocks, cells, channels), jnp.bfloat16),
        in_specs=[hbm] * 6,
        out_specs=pl.BlockSpec(memory_space=pltpu.VMEM),
        scratch_shapes=[
            pltpu.VMEM((cells, channels), jnp.bfloat16),
            pltpu.VMEM((blocks, cells, channels), jnp.bfloat16),
            pltpu.VMEM((blocks, convs, channels), jnp.float32),
            pltpu.VMEM((blocks, convs, channels), jnp.float32),
            pltpu.VMEM((units, outs, depth), jnp.bfloat16),
            pltpu.VMEM((blocks, outs, channels), jnp.bfloat16),
            pltpu.VMEM((channels, channels), jnp.bfloat16),
            pltpu.VMEM((units, batch_n, outs, lanes), jnp.bfloat16),
            pltpu.VMEM((taps, channels, depth), jnp.bfloat16),
            pltpu.VMEM((channels, channels), jnp.bfloat16),
            pltpu.VMEM(((height + taps - 1) * across, depth), jnp.bfloat16),
            pltpu.VMEM((cells, channels), jnp.float32),
            pltpu.VMEM((stages, 2, across, channels), jnp.bfloat16),
            pltpu.VMEM((stages, cells, channels), jnp.bfloat16),
            pltpu.VMEM((stages, 8, channels), jnp.float32),
            pltpu.VMEM((stages, rows_n, 8, channels), jnp.float32),
            dma((7,)),
            dma((1,)), dma((units,)),
            dma((2,)), dma((units,)),
            dma((1,)), dma((units,)),
            dma((1,)), dma((units,)),
            dma((stages, 2)), dma((stages, 2)),
            dma((2,)), dma((stages,)),
        ],
        compiler_params=pltpu.CompilerParams(
            collective_id=0, has_side_effects=True, vmem_limit_bytes=50 * 1024 * 1024),
    )(*(pltpu.with_memory_space_constraint(array, pltpu.HBM) for array in (
        control.reshape(cells, channels),
        unet_skips.reshape(blocks, cells, channels),
        norm_gains,
        norm_shifts,
        conv,
        zero,
    )))
    return out.reshape(blocks, samples, height, across, channels)


def solution(mesh):
    placed = (
        P("batch", "rows", None, None),
        P(None, "batch", "rows", None, None),
        P(),
        P(),
        P(None, None, None, None, "batch"),
        P(None, None, None, "batch"),
    )
    return jax.shard_map(
        functools.partial(on_device, mesh.shape["rows"], mesh.shape["batch"]),
        mesh=mesh,
        in_specs=placed,
        out_specs=P(None, "batch", "rows", None, None),
        check_vma=False,
    )
```
